256 devices in a mesh: gx: 8 (over x, y_lo), gy: 32 (over y_hi, z, core).
Axes of the slice: x: 4, y: 4 (y_hi: 2, y_lo: 2; y = y_hi * 2 + y_lo), z: 8, core: 2. Of those that a mesh axis runs over, the one named last changes fastest.
Arguments:
- density: float32 [256, 1024, 256], P('gx', 'gy'), may hold values from -6 to 6
- flux_east: float32 [256, 1024, 256], P('gx', 'gy'), may hold values from -6 to 6
- flux_north: float32 [256, 1024, 256], P('gx', 'gy'), may hold values from -6 to 6
- flux_up: float32 [256, 1024, 256], P('gx', 'gy'), may hold values from -6 to 6
- theta_pert: float32 [256, 1024, 256], P('gx', 'gy'), may hold values from -2 to 4
- sound_coef: bfloat16 [256, 1024, 256], P('gx', 'gy'), may hold values from 0.5 to 2
- vert_inverse: float32 [512, 512], replicated, may hold values from -1 to 1
Outputs:
- density_new: float32 [256, 1024, 256], P('gx', 'gy')
- east_new: float32 [256, 1024, 256], P('gx', 'gy')
- north_new: float32 [256, 1024, 256], P('gx', 'gy')
- upward_new: float32 [256, 1024, 256], P('gx', 'gy')
- theta_new: float32 [256, 1024, 256], P('gx', 'gy')
The draws below stay inside these ranges and needn't reach their ends.
All inputs are finite; a program needn't handle non-finite values.
Results may differ from the reference program's by a relative error of at most 0.0003.
Values sent between devices are 32-bit elements; how exact they have to be, the bound alone decides.
A program may use at most 64 MiB of HBM per device.

```python
import math
import jax
import jax.numpy as jnp
from jax import lax

NZ = 256
SUBSTEPS = 6
NX = 256
NY = 1024


def draw_theta_pert(key, part):
    return jax.random.truncated_normal(key, -2.0, 4.0, (NX, NY, NZ), jnp.float32)


def draw_vert_inverse(key, part):
    order = 2 * NZ
    spread = 0.25 / math.sqrt(order)
    offdiag = jax.random.truncated_normal(key, -4.0, 4.0, (order, order), jnp.float32) * spread
    return 0.7 * jnp.eye(order, dtype=jnp.float32) + offdiag


def shard_levels(key, dims, shards, low, high):
    loudness, own = 1.0, jax.random.fold_in(key, 6)
    for dim, shards_of in shards:
        draws = jnp.exp(jax.random.uniform(jax.random.fold_in(own, dim), (shards_of,), jnp.float32, low / len(shards), high / len(shards)))
        loudness = loudness * jnp.repeat(draws, dims[dim] // shards_of).reshape([-1 if axis == dim else 1 for axis in range(len(dims))])
    return loudness


def scatter_about(key, extent, scale, limit, cuts=(), kind=jnp.bfloat16):
    entries = jax.random.normal(key, extent, jnp.float32) * scale
    if len(cuts) > 0:
        entries = shard_levels(key, extent, cuts, -0.22, 0.18) * entries
    return jnp.clip(entries, min=-limit, max=limit).astype(kind)


def setup_inputs(seed: int = 0) -> dict:
    arg_keys = jax.random.split(jax.random.key(seed), 8)
    return {
        "density": scatter_about(arg_keys[0], (NX, NY, NZ), 1.0, 6.0, ((0, 8), (1, 32)), jnp.float32),
        "flux_east": scatter_about(arg_keys[1], (NX, NY, NZ), 1.0, 6.0, ((0, 8), (1, 32)), jnp.float32),
        "flux_north": scatter_about(arg_keys[2], (NX, NY, NZ), 1.0, 6.0, ((0, 8), (1, 32)), jnp.float32),
        "flux_up": scatter_about(arg_keys[3], (NX, NY, NZ), 1.0, 6.0, ((0, 8), (1, 32)), jnp.float32),
        "theta_pert": draw_theta_pert(jax.random.fold_in(arg_keys[7], 71), 0),
        "sound_coef": jnp.clip(jnp.exp(math.log(2.0) - 1.3862944 * jax.random.uniform(arg_keys[5], (NX, NY, NZ), jnp.float32) ** shard_levels(arg_keys[5], (NX, NY, NZ), ((0, 8), (1, 32)), -0.2, 0.2)), 0.5, 2.0).astype(jnp.bfloat16),
        "vert_inverse": draw_vert_inverse(jax.random.fold_in(arg_keys[7], 71), 0),
    }


courant = 0.45
damping = 0.1


def reference(density, flux_east, flux_north, flux_up, theta_pert, sound_coef, vert_inverse):
    coef = sound_coef.astype(jnp.float32)
    levels = density.shape[2]
    rho, east, north, upward, theta = density, flux_east, flux_north, flux_up, theta_pert
    divergence = jnp.zeros_like(density)
    for substep in range(SUBSTEPS):
        pressure = coef * theta
        east_next = east - courant * (pressure - jnp.roll(pressure, 1, 0)) + damping * (divergence - jnp.roll(divergence, 1, 0))
        north_next = north - courant * (pressure - jnp.roll(pressure, 1, 1)) + damping * (divergence - jnp.roll(divergence, 1, 1))
        level_div = (jnp.roll(east_next, -1, 0) - east_next) + (jnp.roll(north_next, -1, 1) - north_next)
        right_side = jnp.concatenate([upward, theta - courant * level_div], axis=2)
        shaped = right_side.reshape(-1, 2 * levels)
        solved = jnp.dot(shaped, vert_inverse.T, precision=lax.Precision.HIGHEST, preferred_element_type=jnp.float32)
        solved = solved.reshape(right_side.shape)
        upward = solved[:, :, :levels]
        theta = solved[:, :, levels:]
        below = jnp.concatenate([jnp.zeros_like(upward[:, :, :1]), upward[:, :, :-1]], axis=2)
        divergence = level_div + (upward - below)
        rho = rho - courant * divergence
        east, north = east_next, north_next
    return rho, east, north, upward, theta
```

```python
import jax
import jax.numpy as jnp
from jax import lax
from jax.experimental import pallas as pl
from jax.experimental.pallas import tpu as pltpu
from jax.sharding import PartitionSpec as P

SUBSTEPS = 6
courant = 0.45
damping = 0.1
MESH = pl.DeviceIdType.MESH
f32 = jnp.float32
bf16 = jnp.bfloat16

N = 32
LV = 256
LANES = 128
HALVES = (0, 1)
ROWS = N * N
STRIDE = 40
PADDED = (N + 4) * STRIDE + 8
BX = 4
BR = BX * N
BLOCKS = N // BX
RING = (("x", -1), ("x", N), ("y", -1), ("y", N))
FIRST = (("x", N - 1), ("x", 0), ("y", N - 1), ("y", 0))
SECOND = (("x", N - 2), ("x", 1), ("y", N - 2), ("y", 1))
OUTER = (("x", -2), ("x", N + 1), ("y", -2), ("y", N + 1))
CORNER_FROM = ((N - 1, N - 1), (N - 1, 0), (0, N - 1), (0, 0))
CORNER_AT = ((-1, -1), (-1, N), (N, -1), (N, N))


def lanes(half):
    return pl.ds(half * LANES, LANES)


def row(x, y):
    return (x + 2) * STRIDE + 8 + y


def line(side, dx=0, dy=0):
    axis, at = side
    if axis == "x":
        return pl.ds(row(at + dx, dy), N)
    return pl.ds(row(dx, at + dy), N, STRIDE)


def compact(side):
    axis, at = side
    if axis == "x":
        return pl.ds(at * N, N)
    return pl.ds(at, N, N)


def split(value):
    high = value.astype(bf16)
    return high, (value - high.astype(f32)).astype(bf16)


def kernel(
    rho_h, u_h, v_h, w_h, th_h, cf_h, m_h,
    rho_o, u_o, v_o, w_o, th_o,
    rho, us, vs, ws, th, cf, cc, h0, hh, ms, mh, ml, xh, xl, qs, ga, gb,
    bth, bxh, bxl, bh0, bh, bcc,
    cs, cr, ss, sr, gs, gr, ks, kr,
    lsem, csem, crem, ssem, srem, gsem, grem, ksem, krem,
):
    gx = lax.axis_index("gx")
    gy = lax.axis_index("gy")
    nx = lax.axis_size("gx")
    ny = lax.axis_size("gy")
    xm, xp = lax.rem(gx + nx - 1, nx), lax.rem(gx + 1, nx)
    ym, yp = lax.rem(gy + ny - 1, ny), lax.rem(gy + 1, ny)
    side_to = ((xp, gy), (xm, gy), (gx, yp), (gx, ym))
    corner_to = ((xp, yp), (xp, ym), (xm, yp), (xm, ym))

    loads = []

    def load(src, dst):
        copy = pltpu.make_async_copy(src, dst, lsem.at[len(loads)])
        copy.start()
        loads.append(copy)
        return copy

    load_th = [load(th_h.at[:, lanes(k)], th.at[k]) for k in HALVES]
    load_cf = load(cf_h, cf)
    load_u = [load(u_h.at[:, lanes(k)], us.at[k, pl.ds(0, ROWS)]) for k in HALVES]
    load_v = [load(v_h.at[:, :, lanes(k)], vs.at[k, :, pl.ds(0, N)]) for k in HALVES]
    load_w = [load(w_h.at[:, lanes(k)], ws.at[k]) for k in HALVES]
    load_m = load(m_h, ms)
    load_rho = [load(rho_h.at[:, lanes(k)], rho.at[k]) for k in HALVES]

    barrier = pltpu.get_barrier_semaphore()
    for to in side_to + corner_to:
        pl.semaphore_signal(barrier, inc=1, device_id=to, device_id_type=MESH)

    def grid_of(n):
        return ga if n % 2 == 1 else gb

    vflat = vs.reshape(2, N * STRIDE, LANES)
    for k in HALVES:
        us[k, pl.ds(ROWS, N), :] = jnp.zeros((N, LANES), f32)
        vs[k, :, pl.ds(N, STRIDE - N), :] = jnp.zeros((N, STRIDE - N, LANES), f32)
    ks[...] = jnp.zeros_like(ks)

    for copy in load_th:
        copy.wait()
    load_cf.wait()

    def first_g(b, carry):
        at = pl.ds(pl.multiple_of(b * BR, BR), BR)
        for k in HALVES:
            c = -courant * cf[at, lanes(k)].astype(f32)
            cc[k, at, :] = c
            g = c * th[k, at, :]
            for i in range(BX):
                ga[k, pl.ds(pl.multiple_of((b * BX + i + 2) * STRIDE + 8, 8), N), :] = g[i * N : (i + 1) * N]
        return carry

    lax.fori_loop(0, BLOCKS, first_g, 0)
    for copy in load_u + load_v:
        copy.wait()
    for k in HALVES:
        for s in range(4):
            cs[s, 0, k] = ga[k, line(FIRST[s]), :]
        cs[1, 1, k] = us[k, pl.ds(0, N), :]
        cs[3, 1, k] = vflat[k, pl.ds(0, N, STRIDE), :]
        for c in range(4):
            x, y = CORNER_FROM[c]
            ks[0, c, pl.ds(k, 1), :] = ga[k, pl.ds(row(x, y), 1), :]
            ks[0, c, pl.ds(2 + k, 1), :] = us[k, pl.ds(x * N + y, 1), :]
            ks[0, c, pl.ds(4 + k, 1), :] = vflat[k, pl.ds(x * STRIDE + y, 1), :]

    pl.semaphore_wait(barrier, 8)

    def send(src, dst, sent, got, to):
        return pltpu.make_async_remote_copy(
            src_ref=src, dst_ref=dst, send_sem=sent, recv_sem=got,
            device_id=to, device_id_type=MESH,
        )

    def critical(s):
        part = pl.ds(0, 1 + s % 2)
        return send(cs.at[s, part], cr.at[s, part], csem.at[s], crem.at[s], side_to[s])

    def second(s):
        return send(ss.at[s], sr.at[s], ssem.at[s], srem.at[s], side_to[s])

    def side(slot, s):
        return send(gs.at[slot, s], gr.at[slot, s], gsem.at[slot, s], grem.at[slot, s], side_to[s])

    def corner(slot, c):
        return send(ks.at[slot, c], kr.at[slot, c], ksem.at[slot, c], krem.at[slot, c], corner_to[c])

    for s in range(4):
        critical(s).start()
    for c in range(4):
        corner(0, c).start()

    def first_h(x, carry):
        at = pl.ds(pl.multiple_of(x * N, N), N)
        nxt = pl.ds(pl.multiple_of(x * N + N, N), N)
        for k in HALVES:
            h0[k, at, :] = (us[k, nxt, :] - us[k, at, :]) + (
                vs[k, x, pl.ds(1, N), :] - vs[k, x, pl.ds(0, N), :]
            )
        return carry

    lax.fori_loop(0, N, first_h, 0)
    for copy in load_w:
        copy.wait()
    for k in HALVES:
        for s in range(4):
            edge = compact(FIRST[s])
            ss[s, 0, k] = th[k, edge, :]
            ss[s, 1, k] = ws[k, edge, :]
            ss[s, 2, k] = cc[k, edge, :]
            ss[s, 3, k] = h0[k, edge, :]
            ss[s, 4, k] = ga[k, line(SECOND[s]), :]
    for s in range(4):
        second(s).start()

    def first_w(b, carry):
        at = pl.ds(pl.multiple_of(b * BR, BR), BR)
        for k in HALVES:
            high, low = split(ws[k, at, :])
            xh[at, lanes(k)] = high
            xl[at, lanes(k)] = low
        return carry

    lax.fori_loop(0, BLOCKS, first_w, 0)
    load_m.wait()
    for i in range(4):
        for j in range(4):
            high, low = split(ms[pl.ds(i * 128, 128), pl.ds(j * 128, 128)].T)
            mh[pl.ds(j * 128, 128), pl.ds(i * 128, 128)] = high
            ml[pl.ds(j * 128, 128), pl.ds(i * 128, 128)] = low

    def early_state(s, k):
        at = pl.ds(N * 4 + s * N, N)
        from_main = compact(SECOND[s])
        bth[k, at, :] = th[k, from_main, :]
        bcc[k, at, :] = cc[k, from_main, :]
        high, low = split(ws[k, from_main, :])
        bxh[at, lanes(k)] = high
        bxl[at, lanes(k)] = low

    for k in HALVES:
        for s in range(4):
            early_state(s, k)

    for copy in load_rho:
        copy.wait()
    for s in range(4):
        critical(s).wait_recv()
    for k in HALVES:
        for s in range(4):
            ga[k, line(RING[s]), :] = cr[s, 0, k]
        us[k, pl.ds(ROWS, N), :] = cr[1, 1, k]
        last_x = pl.ds(ROWS - N, N)
        h0[k, last_x, :] = h0[k, last_x, :] + cr[1, 1, k]
        last_y = pl.ds(N - 1, N, N)
        h0[k, last_y, :] = h0[k, last_y, :] + cr[3, 1, k]
        for s in range(4):
            bh0[k, pl.ds(N * 4 + s * N, N), :] = h0[k, compact(SECOND[s]), :]

    first_lane = lax.broadcasted_iota(jnp.int32, (BR, LV), 1) == 0

    def product(high, low):
        q = jnp.dot(high, mh[...], preferred_element_type=f32)
        q = q + jnp.dot(low, mh[...], preferred_element_type=f32)
        return q + jnp.dot(high, ml[...], preferred_element_type=f32)

    def vertical(upward):
        below = jnp.where(first_lane, 0.0, pltpu.roll(upward, 1, 1))
        return upward - below

    def laplacian(grid, k, edge):
        here = grid[k, line(edge), :]
        around = (grid[k, line(edge, -1), :] + grid[k, line(edge, 1), :]) + (
            grid[k, line(edge, 0, -1), :] + grid[k, line(edge, 0, 1), :]
        )
        return around - 4.0 * here, here

    def batch(n, edges, base):
        grid = grid_of(n)
        at = pl.ds(base, 4 * N)
        total = []
        for k in HALVES:
            laps, heres = zip(*[laplacian(grid, k, edge) for edge in edges])
            total.append(jnp.concatenate(heres, axis=0))
            h = bh0[k, at, :] + jnp.concatenate(laps, axis=0)
            bh[k, at, :] = h
            high, low = split(bth[k, at, :] - courant * h)
            bxh[at, pl.ds(LV + k * LANES, LANES)] = high
            bxl[at, pl.ds(LV + k * LANES, LANES)] = low
        q = product(bxh[at, :], bxl[at, :])
        diff = vertical(q[:, :LV])
        out = []
        for k in HALVES:
            part = slice(k * LANES, (k + 1) * LANES)
            high, low = split(q[:, part])
            bxh[at, lanes(k)] = high
            bxl[at, lanes(k)] = low
            theta = q[:, LV + k * LANES : LV + (k + 1) * LANES]
            bth[k, at, :] = theta
            div = bh[k, at, :] + diff[:, part]
            out.append(total[k] + bcc[k, at, :] * theta + damping * div)
        return out

    def early(n, slot):
        out = batch(n, SECOND, 4 * N)
        for k in HALVES:
            for s in range(4):
                gs[slot, s, k] = out[k][s * N : (s + 1) * N]
        for s in range(4):
            side(slot, s).start()

    def ring(n):
        out = batch(n, RING, 0)
        grid = grid_of(n + 1)
        for k in HALVES:
            for s in range(4):
                grid[k, line(RING[s]), :] = out[k][s * N : (s + 1) * N]

    def ring_state():
        for s in range(4):
            second(s).wait_recv()
        for c in range(4):
            corner(0, c).wait_recv()
        last = lax.broadcasted_iota(jnp.int32, (N, LANES), 0) == N - 1
        for k in HALVES:
            extra = (
                us[k, pl.ds(0, N), :], None, vflat[k, pl.ds(0, N, STRIDE), :], None,
            )
            end = (kr[0, 1, pl.ds(4 + k, 1), :], kr[0, 3, pl.ds(4 + k, 1), :],
                   kr[0, 2, pl.ds(2 + k, 1), :], kr[0, 3, pl.ds(2 + k, 1), :])
            for s in range(4):
                at = pl.ds(s * N, N)
                bth[k, at, :] = sr[s, 0, k]
                high, low = split(sr[s, 1, k])
                bxh[at, lanes(k)] = high
                bxl[at, lanes(k)] = low
                bcc[k, at, :] = sr[s, 2, k]
                h = sr[s, 3, k] + jnp.where(last, end[s], 0.0)
                bh0[k, at, :] = h if extra[s] is None else h + extra[s]
                ga[k, line(OUTER[s]), :] = sr[s, 4, k]
                x, y = CORNER_AT[s]
                ga[k, pl.ds(row(x, y), 1), :] = kr[0, s, pl.ds(k, 1), :]

    def receive(n, slot):
        grid = grid_of(n)
        for s in range(4):
            side(slot, s).wait_recv()
            corner(slot + 1, s).wait_recv()
        for k in HALVES:
            for s in range(4):
                grid[k, line(OUTER[s]), :] = gr[slot, s, k]
                x, y = CORNER_AT[s]
                grid[k, pl.ds(row(x, y), 1), :] = kr[slot + 1, s, pl.ds(k, 1), :]

    def prepare(n, b):
        grid = grid_of(n)
        at = pl.ds(b * BR, BR)
        for k in HALVES:
            laps = []
            for i in range(BX):
                lap, here = laplacian(grid, k, ("x", b * BX + i))
                laps.append(lap)
                if n == SUBSTEPS:
                    x = b * BX + i
                    west = grid[k, pl.ds(row(x - 1, 0), N), :]
                    south = grid[k, pl.ds(row(x, -1), N), :]
                    own = pl.ds(x * N, N)
                    u_o[own, lanes(k)] = us[k, own, :] + (here - west)
                    v_o[own, lanes(k)] = vs[k, x, pl.ds(0, N), :] + (here - south)
            h = h0[k, at, :] + jnp.concatenate(laps, axis=0)
            hh[k, at, :] = h
            high, low = split(th[k, at, :] - courant * h)
            xh[at, pl.ds(LV + k * LANES, LANES)] = high
            xl[at, pl.ds(LV + k * LANES, LANES)] = low

    def multiply(b):
        at = pl.ds(b * BR, BR)
        qs[b % 2] = product(xh[at, :], xl[at, :])

    def finish(n, b):
        at = pl.ds(b * BR, BR)
        upward = qs[b % 2, :, pl.ds(0, LV)]
        diff = vertical(upward)
        for k in HALVES:
            part = slice(k * LANES, (k + 1) * LANES)
            theta = qs[b % 2, :, pl.ds(LV + k * LANES, LANES)]
            div = hh[k, at, :] + diff[:, part]
            density = rho[k, at, :] - courant * div
            if n == SUBSTEPS:
                rho_o[at, lanes(k)] = density
                w_o[at, lanes(k)] = upward[:, part]
                th_o[at, lanes(k)] = theta
                continue
            rho[k, at, :] = density
            th[k, at, :] = theta
            high, low = split(upward[:, part])
            xh[at, lanes(k)] = high
            xl[at, lanes(k)] = low
            g = cc[k, at, :] * theta + damping * div
            for i in range(BX):
                own = pl.ds(row(b * BX + i, 0), N)
                grid_of(n + 1)[k, own, :] = grid_of(n)[k, own, :] + g[i * N : (i + 1) * N]

    def main(n):
        prepare(n, 0)
        for b in range(BLOCKS):
            if b + 1 < BLOCKS:
                prepare(n, b + 1)
            multiply(b)
            if b > 0:
                finish(n, b - 1)
        finish(n, BLOCKS - 1)

    def corners(n, slot):
        grid = grid_of(n)
        for c in range(4):
            x, y = CORNER_FROM[c]
            for k in HALVES:
                ks[slot, c, pl.ds(k, 1), :] = grid[k, pl.ds(row(x, y), 1), :]
        for c in range(4):
            corner(slot, c).start()

    early(1, 0)
    main(1)
    corners(2, 1)
    ring_state()
    ring(1)

    def pair(i, carry):
        for n in (2, 3):
            slot = 2 * i + n - 2
            early(n, slot + 1)
            main(n)
            corners(n + 1, slot + 2)
            receive(n, slot)
            ring(n)
        return carry

    lax.fori_loop(0, 2, pair, 0)
    main(SUBSTEPS)

    for s in range(4):
        side(4, s).wait_recv()
        corner(5, s).wait_recv()
        critical(s).wait_send()
        second(s).wait_send()
        corner(0, s).wait_send()
        for slot in range(5):
            side(slot, s).wait_send()
            corner(slot + 1, s).wait_send()


def body(density, flux_east, flux_north, flux_up, theta_pert, sound_coef, vert_inverse):
    flat = (ROWS, LV)
    half = pltpu.VMEM((2, ROWS, LANES), f32)
    plane = (2, N, LANES)
    any_space = pl.BlockSpec(memory_space=pl.ANY)
    vmem = pl.BlockSpec(memory_space=pltpu.VMEM)
    dma = pltpu.SemaphoreType.DMA
    outs = pl.pallas_call(
        kernel,
        out_shape=[jax.ShapeDtypeStruct(flat, f32)] * 5,
        in_specs=[any_space] * 7,
        out_specs=[vmem] * 5,
        scratch_shapes=[
            half,
            pltpu.VMEM((2, ROWS + N, LANES), f32),
            pltpu.VMEM((2, N, STRIDE, LANES), f32),
            half,
            half,
            pltpu.VMEM(flat, bf16),
            half,
            half,
            half,
            pltpu.VMEM((2 * LV, 2 * LV), f32),
            pltpu.VMEM((2 * LV, 2 * LV), bf16),
            pltpu.VMEM((2 * LV, 2 * LV), bf16),
            pltpu.VMEM((ROWS, 2 * LV), bf16),
            pltpu.VMEM((ROWS, 2 * LV), bf16),
            pltpu.VMEM((2, BR, 2 * LV), f32),
            pltpu.VMEM((2, PADDED, LANES), f32),
            pltpu.VMEM((2, PADDED, LANES), f32),
            pltpu.VMEM((2, 8 * N, LANES), f32),
            pltpu.VMEM((8 * N, 2 * LV), bf16),
            pltpu.VMEM((8 * N, 2 * LV), bf16),
            pltpu.VMEM((2, 8 * N, LANES), f32),
            pltpu.VMEM((2, 8 * N, LANES), f32),
            pltpu.VMEM((2, 8 * N, LANES), f32),
            pltpu.VMEM((4, 2) + plane, f32),
            pltpu.VMEM((4, 2) + plane, f32),
            pltpu.VMEM((4, 5) + plane, f32),
            pltpu.VMEM((4, 5) + plane, f32),
            pltpu.VMEM((5, 4) + plane, f32),
            pltpu.VMEM((5, 4) + plane, f32),
            pltpu.VMEM((6, 4, 8, LANES), f32),
            pltpu.VMEM((6, 4, 8, LANES), f32),
            dma((12,)),
            dma((4,)), dma((4,)),
            dma((4,)), dma((4,)),
            dma((5, 4)), dma((5, 4)),
            dma((6, 4)), dma((6, 4)),
        ],
        compiler_params=pltpu.CompilerParams(
            collective_id=0, has_side_effects=True, vmem_limit_bytes=50 * 1024 * 1024
        ),
    )(
        density.reshape(flat),
        flux_east.reshape(flat),
        flux_north,
        flux_up.reshape(flat),
        theta_pert.reshape(flat),
        sound_coef.reshape(flat),
        vert_inverse,
    )
    return tuple(out.reshape(N, N, LV) for out in outs)


def solution(mesh):
    block = P("gx", "gy", None)
    return jax.shard_map(
        body,
        mesh=mesh,
        in_specs=(block,) * 6 + (P(),),
        out_specs=(block,) * 5,
        check_vma=False,
    )
```

```python
import jax
import jax.numpy as jnp
from jax import lax
from jax.experimental import pallas as pl
from jax.experimental.pallas import tpu as pltpu
from jax.sharding import PartitionSpec as P

SUBSTEPS = 6
courant = 0.45
damping = 0.1
MESH = pl.DeviceIdType.MESH
f32 = jnp.float32
bf16 = jnp.bfloat16

N = 32
LV = 256
LANES = 128
HALVES = (0, 1)
ROWS = N * N
STRIDE = 40
PADDED = (N + 4) * STRIDE + 8
BX = 4
BR = BX * N
BLOCKS = N // BX
CORNER_ROWS = 16
RING = (("x", -1), ("x", N), ("y", -1), ("y", N))
FIRST = (("x", N - 1), ("x", 0), ("y", N - 1), ("y", 0))
SECOND = (("x", N - 2), ("x", 1), ("y", N - 2), ("y", 1))
OUTER = (("x", -2), ("x", N + 1), ("y", -2), ("y", N + 1))
CORNER_FROM = ((N - 1, N - 1), (N - 1, 0), (0, N - 1), (0, 0))
CORNER_AT = ((-1, -1), (-1, N), (N, -1), (N, N))


def lanes(half):
    return pl.ds(half * LANES, LANES)


def row(x, y):
    return (x + 2) * STRIDE + 8 + y


def line(side, dx=0, dy=0):
    axis, at = side
    if axis == "x":
        return pl.ds(row(at + dx, dy), N)
    return pl.ds(row(dx, at + dy), N, STRIDE)


def compact(side):
    axis, at = side
    if axis == "x":
        return pl.ds(at * N, N)
    return pl.ds(at, N, N)


def split(value):
    high = value.astype(bf16)
    return high, (value - high.astype(f32)).astype(bf16)


def vertical(upward):
    first = lax.broadcasted_iota(jnp.int32, upward.shape, 1) == 0
    return upward - jnp.where(first, 0.0, pltpu.roll(upward, 1, 1))


def laplacian(grid, k, edge):
    here = grid[k, line(edge), :]
    around = (grid[k, line(edge, -1), :] + grid[k, line(edge, 1), :]) + (
        grid[k, line(edge, 0, -1), :] + grid[k, line(edge, 0, 1), :]
    )
    return around - 4.0 * here, here


def corner_laplacian(grid, k, x, y):
    at = [grid[k, pl.ds(row(x + i, y + j), 1), :] for i, j in ((0, 0), (-1, 0), (1, 0), (0, -1), (0, 1))]
    return (at[1] + at[2]) + (at[3] + at[4]) - 4.0 * at[0], at[0]


def corner_rows(rows):
    return jnp.concatenate(rows + [jnp.zeros((CORNER_ROWS - 4, LANES), f32)], axis=0)


def product(mh, ml, parts):
    total = None
    for high, low, depth in parts:
        for left, right in ((high, mh), (low, mh), (high, ml)):
            term = jnp.dot(left, right[depth, :], preferred_element_type=f32)
            total = term if total is None else total + term
    return total


def pipeline(grid, h0, th, hh, tth, ttl, wh, wl, mh, ml, qs, finish, extra=None):
    def prepare(b):
        at = pl.ds(b * BR, BR)
        for k in HALVES:
            laps = []
            for i in range(BX):
                lap, here = laplacian(grid, k, ("x", b * BX + i))
                laps.append(lap)
                if extra is not None:
                    extra(k, b * BX + i, here)
            h = h0[k, at, :] + jnp.concatenate(laps, axis=0)
            hh[k, at, :] = h
            high, low = split(th[k, at, :] - courant * h)
            tth[at, lanes(k)] = high
            ttl[at, lanes(k)] = low

    def multiply(b):
        at = pl.ds(b * BR, BR)
        qs[b % 2] = product(mh, ml, [
            (wh[at, :], wl[at, :], pl.ds(0, LV)),
            (tth[at, :], ttl[at, :], pl.ds(LV, LV)),
        ])

    prepare(0)
    for b in range(BLOCKS):
        if b + 1 < BLOCKS:
            prepare(b + 1)
        multiply(b)
        if b > 0:
            finish(b - 1)
    finish(BLOCKS - 1)


def last_kernel(
    rho, us, vs, th, h0, mh, ml, wh, wl, grid,
    rho_h, u_h, v_h, w_h, th_h,
    rho_o, u_o, v_o, w_o, th_o, hh, tth, ttl, qs, sem,
):
    copies = []

    def store(src, dst, b):
        at = pl.ds(b * BR, BR)
        copy = pltpu.make_async_copy(src.at[at], dst.at[at], sem.at[len(copies)])
        copy.start()
        copies.append(copy)

    def extra(k, x, here):
        own = pl.ds(x * N, N)
        west = grid[k, pl.ds(row(x - 1, 0), N), :]
        south = grid[k, pl.ds(row(x, -1), N), :]
        u_o[own, lanes(k)] = us[k, own, :] + (here - west)
        v_o[own, lanes(k)] = vs[k, x, pl.ds(0, N), :] + (here - south)

    def finish(b):
        at = pl.ds(b * BR, BR)
        upward = qs[b % 2, :, pl.ds(0, LV)]
        diff = vertical(upward)
        w_o[at, :] = upward
        th_o[at, :] = qs[b % 2, :, pl.ds(LV, LV)]
        for k in HALVES:
            div = hh[k, at, :] + diff[:, k * LANES : (k + 1) * LANES]
            rho_o[at, lanes(k)] = rho[k, at, :] - courant * div
        store(u_o, u_h, b)
        store(v_o, v_h, b)
        store(rho_o, rho_h, b)
        store(w_o, w_h, b)
        store(th_o, th_h, b)

    pipeline(grid, h0, th, hh, tth, ttl, wh, wl, mh, ml, qs, finish, extra)
    for copy in copies:
        copy.wait()


def kernel(
    rho_h, u_h, v_h, w_h, th_h, cf_h, m_h,
    rho, us, vs, th, h0, mh, ml, wh, wl, gb,
    ws, cf, cc, hh, ms, tth, ttl, qs, ga,
    bth, bxh, bxl, bh0, bh, bcc,
    cs, cr, ss, sr, gs, gr, ks, kr,
    lsem, csem, crem, ssem, srem, gsem, grem, ksem, krem,
):
    gx = lax.axis_index("gx")
    gy = lax.axis_index("gy")
    nx = lax.axis_size("gx")
    ny = lax.axis_size("gy")
    xm, xp = lax.rem(gx + nx - 1, nx), lax.rem(gx + 1, nx)
    ym, yp = lax.rem(gy + ny - 1, ny), lax.rem(gy + 1, ny)
    side_to = ((xp, gy), (xm, gy), (gx, yp), (gx, ym))
    corner_to = ((xp, yp), (xp, ym), (xm, yp), (xm, ym))

    loads = []

    def load(src, dst):
        copy = pltpu.make_async_copy(src, dst, lsem.at[len(loads)])
        copy.start()
        loads.append(copy)
        return copy

    load_th = [load(th_h.at[:, lanes(k)], th.at[k]) for k in HALVES]
    load_cf = load(cf_h, cf)
    load_u = [load(u_h.at[:, lanes(k)], us.at[k, pl.ds(0, ROWS)]) for k in HALVES]
    load_v = [load(v_h.at[:, :, lanes(k)], vs.at[k, :, pl.ds(0, N)]) for k in HALVES]
    load_w = [load(w_h.at[:, lanes(k)], ws.at[k]) for k in HALVES]
    load_m = load(m_h, ms)
    load_rho = [load(rho_h.at[:, lanes(k)], rho.at[k]) for k in HALVES]

    barrier = pltpu.get_barrier_semaphore()
    for to in side_to + corner_to:
        pl.semaphore_signal(barrier, inc=1, device_id=to, device_id_type=MESH)

    def grid_of(n):
        return ga if n % 2 == 1 else gb

    vflat = vs.reshape(2, N * STRIDE, LANES)
    for k in HALVES:
        us[k, pl.ds(ROWS, N), :] = jnp.zeros((N, LANES), f32)
        vs[k, :, pl.ds(N, STRIDE - N), :] = jnp.zeros((N, STRIDE - N, LANES), f32)
    ks[...] = jnp.zeros_like(ks)

    for copy in load_th:
        copy.wait()
    load_cf.wait()

    def first_g(b, carry):
        at = pl.ds(pl.multiple_of(b * BR, BR), BR)
        for k in HALVES:
            c = -courant * cf[at, lanes(k)].astype(f32)
            cc[k, at, :] = c
            g = c * th[k, at, :]
            for i in range(BX):
                ga[k, pl.ds(pl.multiple_of((b * BX + i + 2) * STRIDE + 8, 8), N), :] = g[i * N : (i + 1) * N]
        return carry

    lax.fori_loop(0, BLOCKS, first_g, 0)
    for copy in load_u + load_v:
        copy.wait()
    for k in HALVES:
        for s in range(4):
            cs[s, 0, k] = ga[k, line(FIRST[s]), :]
        cs[1, 1, k] = us[k, pl.ds(0, N), :]
        cs[3, 1, k] = vflat[k, pl.ds(0, N, STRIDE), :]
        for c in range(4):
            x, y = CORNER_FROM[c]
            ks[0, c, pl.ds(k, 1), :] = ga[k, pl.ds(row(x, y), 1), :]
            ks[0, c, pl.ds(2 + k, 1), :] = us[k, pl.ds(x * N + y, 1), :]
            ks[0, c, pl.ds(4 + k, 1), :] = vflat[k, pl.ds(x * STRIDE + y, 1), :]

    pl.semaphore_wait(barrier, 8)

    def send(src, dst, sent, got, to):
        return pltpu.make_async_remote_copy(
            src_ref=src, dst_ref=dst, send_sem=sent, recv_sem=got,
            device_id=to, device_id_type=MESH,
        )

    def critical(s):
        part = pl.ds(0, 1 + s % 2)
        return send(cs.at[s, part], cr.at[s, part], csem.at[s], crem.at[s], side_to[s])

    def second(s):
        return send(ss.at[s], sr.at[s], ssem.at[s], srem.at[s], side_to[s])

    def side(slot, s):
        return send(gs.at[slot, s], gr.at[slot, s], gsem.at[slot, s], grem.at[slot, s], side_to[s])

    def corner(slot, c):
        return send(ks.at[slot, c], kr.at[slot, c], ksem.at[slot, c], krem.at[slot, c], corner_to[c])

    for s in range(4):
        critical(s).start()
    for c in range(4):
        corner(0, c).start()

    def first_h(x, carry):
        at = pl.ds(pl.multiple_of(x * N, N), N)
        nxt = pl.ds(pl.multiple_of(x * N + N, N), N)
        for k in HALVES:
            h0[k, at, :] = (us[k, nxt, :] - us[k, at, :]) + (
                vs[k, x, pl.ds(1, N), :] - vs[k, x, pl.ds(0, N), :]
            )
        return carry

    lax.fori_loop(0, N, first_h, 0)
    for copy in load_w:
        copy.wait()
    for k in HALVES:
        for s in range(4):
            edge = compact(FIRST[s])
            ss[s, 0, k] = th[k, edge, :]
            ss[s, 1, k] = ws[k, edge, :]
            ss[s, 2, k] = cc[k, edge, :]
            ss[s, 3, k] = h0[k, edge, :]
            ss[s, 4, k] = ga[k, line(SECOND[s]), :]
    for s in range(4):
        second(s).start()

    def first_w(b, carry):
        at = pl.ds(pl.multiple_of(b * BR, BR), BR)
        for k in HALVES:
            high, low = split(ws[k, at, :])
            wh[at, lanes(k)] = high
            wl[at, lanes(k)] = low
        return carry

    lax.fori_loop(0, BLOCKS, first_w, 0)
    load_m.wait()
    for i in range(4):
        for j in range(4):
            high, low = split(ms[pl.ds(i * 128, 128), pl.ds(j * 128, 128)].T)
            mh[pl.ds(j * 128, 128), pl.ds(i * 128, 128)] = high
            ml[pl.ds(j * 128, 128), pl.ds(i * 128, 128)] = low

    own_corners = [pl.ds(x * N + y, 1) for x, y in CORNER_FROM]

    def early_state(s, k):
        at = pl.ds(N * 4 + s * N, N)
        from_main = compact(SECOND[s])
        bth[k, at, :] = th[k, from_main, :]
        bcc[k, at, :] = cc[k, from_main, :]
        high, low = split(ws[k, from_main, :])
        bxh[at, lanes(k)] = high
        bxl[at, lanes(k)] = low

    for k in HALVES:
        for s in range(4):
            early_state(s, k)
        at = pl.ds(8 * N, CORNER_ROWS)
        bth[k, at, :] = corner_rows([th[k, own, :] for own in own_corners])
        bcc[k, at, :] = corner_rows([cc[k, own, :] for own in own_corners])
        high, low = split(corner_rows([ws[k, own, :] for own in own_corners]))
        bxh[at, lanes(k)] = high
        bxl[at, lanes(k)] = low

    for copy in load_rho:
        copy.wait()
    for s in range(4):
        critical(s).wait_recv()
    for k in HALVES:
        for s in range(4):
            ga[k, line(RING[s]), :] = cr[s, 0, k]
        us[k, pl.ds(ROWS, N), :] = cr[1, 1, k]
        last_x = pl.ds(ROWS - N, N)
        h0[k, last_x, :] = h0[k, last_x, :] + cr[1, 1, k]
        last_y = pl.ds(N - 1, N, N)
        h0[k, last_y, :] = h0[k, last_y, :] + cr[3, 1, k]
        for s in range(4):
            bh0[k, pl.ds(N * 4 + s * N, N), :] = h0[k, compact(SECOND[s]), :]
        bh0[k, pl.ds(8 * N, CORNER_ROWS), :] = corner_rows([h0[k, own, :] for own in own_corners])

    def batch(n, edges, base, with_corners):
        grid = grid_of(n)
        at = pl.ds(base, 4 * N + (CORNER_ROWS if with_corners else 0))
        total = []
        for k in HALVES:
            laps, heres = zip(*[laplacian(grid, k, edge) for edge in edges])
            if with_corners:
                more = [corner_laplacian(grid, k, x, y) for x, y in CORNER_FROM]
                laps += (corner_rows([lap for lap, _ in more]),)
                heres += (corner_rows([here for _, here in more]),)
            total.append(jnp.concatenate(heres, axis=0))
            h = bh0[k, at, :] + jnp.concatenate(laps, axis=0)
            bh[k, at, :] = h
            high, low = split(bth[k, at, :] - courant * h)
            bxh[at, pl.ds(LV + k * LANES, LANES)] = high
            bxl[at, pl.ds(LV + k * LANES, LANES)] = low
        q = product(mh, ml, [(bxh[at, :], bxl[at, :], pl.ds(0, 2 * LV))])
        diff = vertical(q[:, :LV])
        out = []
        for k in HALVES:
            part = slice(k * LANES, (k + 1) * LANES)
            high, low = split(q[:, part])
            bxh[at, lanes(k)] = high
            bxl[at, lanes(k)] = low
            theta = q[:, LV + k * LANES : LV + (k + 1) * LANES]
            bth[k, at, :] = theta
            div = bh[k, at, :] + diff[:, part]
            out.append(total[k] + bcc[k, at, :] * theta + damping * div)
        return out

    def early(n, slot):
        out = batch(n, SECOND, 4 * N, True)
        for k in HALVES:
            for s in range(4):
                gs[slot, s, k] = out[k][s * N : (s + 1) * N]
                ks[slot + 1, s, pl.ds(k, 1), :] = out[k][4 * N + s : 4 * N + s + 1]
        for s in range(4):
            side(slot, s).start()
            corner(slot + 1, s).start()

    def ring(n):
        out = batch(n, RING, 0, False)
        grid = grid_of(n + 1)
        for k in HALVES:
            for s in range(4):
                grid[k, line(RING[s]), :] = out[k][s * N : (s + 1) * N]

    def ring_state():
        for s in range(4):
            second(s).wait_recv()
        for c in range(4):
            corner(0, c).wait_recv()
        last = lax.broadcasted_iota(jnp.int32, (N, LANES), 0) == N - 1
        for k in HALVES:
            extra = (
                us[k, pl.ds(0, N), :], None, vflat[k, pl.ds(0, N, STRIDE), :], None,
            )
            end = (kr[0, 1, pl.ds(4 + k, 1), :], kr[0, 3, pl.ds(4 + k, 1), :],
                   kr[0, 2, pl.ds(2 + k, 1), :], kr[0, 3, pl.ds(2 + k, 1), :])
            for s in range(4):
                at = pl.ds(s * N, N)
                bth[k, at, :] = sr[s, 0, k]
                high, low = split(sr[s, 1, k])
                bxh[at, lanes(k)] = high
                bxl[at, lanes(k)] = low
                bcc[k, at, :] = sr[s, 2, k]
                h = sr[s, 3, k] + jnp.where(last, end[s], 0.0)
                bh0[k, at, :] = h if extra[s] is None else h + extra[s]
                ga[k, line(OUTER[s]), :] = sr[s, 4, k]
                x, y = CORNER_AT[s]
                ga[k, pl.ds(row(x, y), 1), :] = kr[0, s, pl.ds(k, 1), :]

    def receive(n, slot):
        grid = grid_of(n)
        for s in range(4):
            side(slot, s).wait_recv()
            corner(slot + 1, s).wait_recv()
        for k in HALVES:
            for s in range(4):
                grid[k, line(OUTER[s]), :] = gr[slot, s, k]
                x, y = CORNER_AT[s]
                grid[k, pl.ds(row(x, y), 1), :] = kr[slot + 1, s, pl.ds(k, 1), :]

    def main(n):
        grid, later = grid_of(n), grid_of(n + 1)

        def finish(b):
            at = pl.ds(b * BR, BR)
            upward = qs[b % 2, :, pl.ds(0, LV)]
            diff = vertical(upward)
            for k in HALVES:
                part = slice(k * LANES, (k + 1) * LANES)
                theta = qs[b % 2, :, pl.ds(LV + k * LANES, LANES)]
                div = hh[k, at, :] + diff[:, part]
                rho[k, at, :] = rho[k, at, :] - courant * div
                th[k, at, :] = theta
                high, low = split(upward[:, part])
                wh[at, lanes(k)] = high
                wl[at, lanes(k)] = low
                g = cc[k, at, :] * theta + damping * div
                for i in range(BX):
                    own = pl.ds(row(b * BX + i, 0), N)
                    later[k, own, :] = grid[k, own, :] + g[i * N : (i + 1) * N]

        pipeline(grid, h0, th, hh, tth, ttl, wh, wl, mh, ml, qs, finish)

    early(1, 0)
    main(1)
    ring_state()
    ring(1)

    def pair(i, carry):
        for n in (2, 3):
            slot = 2 * i + n - 2
            early(n, slot + 1)
            main(n)
            receive(n, slot)
            ring(n)
        return carry

    lax.fori_loop(0, 2, pair, 0)

    for s in range(4):
        side(4, s).wait_recv()
        corner(5, s).wait_recv()
        critical(s).wait_send()
        second(s).wait_send()
        corner(0, s).wait_send()
        for slot in range(5):
            side(slot, s).wait_send()
            corner(slot + 1, s).wait_send()


def body(density, flux_east, flux_north, flux_up, theta_pert, sound_coef, vert_inverse):
    flat = (ROWS, LV)
    half_shape = (2, ROWS, LANES)
    half = pltpu.VMEM(half_shape, f32)
    operand = pltpu.VMEM(flat, bf16)
    plane = (2, N, LANES)
    batch_half = pltpu.VMEM((2, 8 * N + CORNER_ROWS, LANES), f32)
    batch_operand = pltpu.VMEM((8 * N + CORNER_ROWS, 2 * LV), bf16)
    hbm = pl.BlockSpec(memory_space=pltpu.HBM)
    vmem = pl.BlockSpec(memory_space=pltpu.VMEM)
    dma = pltpu.SemaphoreType.DMA
    shape = jax.ShapeDtypeStruct
    state = pl.pallas_call(
        kernel,
        out_shape=[
            shape(half_shape, f32),
            shape((2, ROWS + N, LANES), f32),
            shape((2, N, STRIDE, LANES), f32),
            shape(half_shape, f32),
            shape(half_shape, f32),
            shape((2 * LV, 2 * LV), bf16),
            shape((2 * LV, 2 * LV), bf16),
            shape(flat, bf16),
            shape(flat, bf16),
            shape((2, PADDED, LANES), f32),
        ],
        in_specs=[hbm] * 7,
        out_specs=[vmem] * 10,
        scratch_shapes=[
            half,
            operand,
            half,
            half,
            pltpu.VMEM((2 * LV, 2 * LV), f32),
            operand,
            operand,
            pltpu.VMEM((2, BR, 2 * LV), f32),
            pltpu.VMEM((2, PADDED, LANES), f32),
            batch_half,
            batch_operand,
            batch_operand,
            batch_half,
            batch_half,
            batch_half,
            pltpu.VMEM((4, 2) + plane, f32),
            pltpu.VMEM((4, 2) + plane, f32),
            pltpu.VMEM((4, 5) + plane, f32),
            pltpu.VMEM((4, 5) + plane, f32),
            pltpu.VMEM((5, 4) + plane, f32),
            pltpu.VMEM((5, 4) + plane, f32),
            pltpu.VMEM((6, 4, 8, LANES), f32),
            pltpu.VMEM((6, 4, 8, LANES), f32),
            dma((12,)),
            dma((4,)), dma((4,)),
            dma((4,)), dma((4,)),
            dma((5, 4)), dma((5, 4)),
            dma((6, 4)), dma((6, 4)),
        ],
        compiler_params=pltpu.CompilerParams(
            collective_id=0, has_side_effects=True, vmem_limit_bytes=28 * 1024 * 1024
        ),
    )(*[pltpu.with_memory_space_constraint(array, pltpu.HBM) for array in (
        density.reshape(flat),
        flux_east.reshape(flat),
        flux_north,
        flux_up.reshape(flat),
        theta_pert.reshape(flat),
        sound_coef.reshape(flat),
        vert_inverse,
    )])
    out = pltpu.VMEM(flat, f32)
    outs = pl.pallas_call(
        last_kernel,
        out_shape=[shape(flat, f32)] * 5,
        in_specs=[vmem] * 10,
        out_specs=[hbm] * 5,
        scratch_shapes=[
            out, out, out, out, out, half, operand, operand,
            pltpu.VMEM((2, BR, 2 * LV), f32),
            dma((5 * BLOCKS,)),
        ],
        compiler_params=pltpu.CompilerParams(vmem_limit_bytes=28 * 1024 * 1024),
    )(*state)
    return tuple(out.reshape(N, N, LV) for out in outs)


def solution(mesh):
    block = P("gx", "gy", None)
    return jax.shard_map(
        body,
        mesh=mesh,
        in_specs=(block,) * 6 + (P(),),
        out_specs=(block,) * 5,
        check_vma=False,
    )
```

```python
import jax
import jax.numpy as jnp
from jax import lax
from jax.experimental import pallas as pl
from jax.experimental.pallas import tpu as pltpu
from jax.sharding import PartitionSpec as P

SUBSTEPS = 6
courant = 0.45
damping = 0.1
MESH = pl.DeviceIdType.MESH
f32 = jnp.float32
bf16 = jnp.bfloat16

N = 32
LV = 256
LANES = 128
HALVES = (0, 1)
ROWS = N * N
STRIDE = 40
PADDED = (N + 4) * STRIDE + 8
BX = 4
BR = BX * N
BLOCKS = N // BX
CORNER_ROWS = 16
MESSAGES = SUBSTEPS - 2
RING = (("x", -1), ("x", N), ("y", -1), ("y", N))
FIRST = (("x", N - 1), ("x", 0), ("y", N - 1), ("y", 0))
SECOND = (("x", N - 2), ("x", 1), ("y", N - 2), ("y", 1))
OUTER = (("x", -2), ("x", N + 1), ("y", -2), ("y", N + 1))
CORNER_FROM = ((N - 1, N - 1), (N - 1, 0), (0, N - 1), (0, 0))
CORNER_AT = ((-1, -1), (-1, N), (N, -1), (N, N))


def lanes(half):
    return pl.ds(half * LANES, LANES)


def row(x, y):
    return (x + 2) * STRIDE + 8 + y


def line(side, dx=0, dy=0):
    axis, at = side
    if axis == "x":
        return pl.ds(row(at + dx, dy), N)
    return pl.ds(row(dx, at + dy), N, STRIDE)


def compact(side):
    axis, at = side
    if axis == "x":
        return pl.ds(at * N, N)
    return pl.ds(at, N, N)


def split(value):
    high = value.astype(bf16)
    return high, (value - high.astype(f32)).astype(bf16)


def vertical(upward):
    first = lax.broadcasted_iota(jnp.int32, upward.shape, 1) == 0
    return upward - jnp.where(first, 0.0, pltpu.roll(upward, 1, 1))


def laplacian(grid, k, edge):
    here = grid[k, line(edge), :]
    around = (grid[k, line(edge, -1), :] + grid[k, line(edge, 1), :]) + (
        grid[k, line(edge, 0, -1), :] + grid[k, line(edge, 0, 1), :]
    )
    return around - 4.0 * here, here


def corner_laplacian(grid, k, x, y):
    at = [grid[k, pl.ds(row(x + i, y + j), 1), :] for i, j in ((0, 0), (-1, 0), (1, 0), (0, -1), (0, 1))]
    return (at[1] + at[2]) + (at[3] + at[4]) - 4.0 * at[0], at[0]


def corner_rows(rows):
    return jnp.concatenate(rows + [jnp.zeros((CORNER_ROWS - 4, LANES), f32)], axis=0)


def product(mh, ml, parts):
    total = None
    for high, low, depth in parts:
        for left, right in ((high, mh), (low, mh), (high, ml)):
            term = jnp.dot(left, right[depth, :], preferred_element_type=f32)
            total = term if total is None else total + term
    return total


def pipeline(grid, h0, th, hh, tth, ttl, wh, wl, mh, ml, qs, finish, extra=None):
    def prepare(b):
        at = pl.ds(b * BR, BR)
        for k in HALVES:
            laps = []
            for i in range(BX):
                lap, here = laplacian(grid, k, ("x", b * BX + i))
                laps.append(lap)
                if extra is not None:
                    extra(k, b * BX + i, here)
            h = h0[k, at, :] + jnp.concatenate(laps, axis=0)
            hh[k, at, :] = h
            high, low = split(th[k, at, :] - courant * h)
            tth[at, lanes(k)] = high
            ttl[at, lanes(k)] = low

    def multiply(b):
        at = pl.ds(b * BR, BR)
        qs[b % 2] = product(mh, ml, [
            (wh[at, :], wl[at, :], pl.ds(0, LV)),
            (tth[at, :], ttl[at, :], pl.ds(LV, LV)),
        ])

    prepare(0)
    for b in range(BLOCKS):
        if b + 1 < BLOCKS:
            prepare(b + 1)
        multiply(b)
        if b > 0:
            finish(b - 1)
    finish(BLOCKS - 1)


def last_kernel(
    rho, us, vs, th, h0, mh, ml, wh, wl, grid,
    rho_h, u_h, v_h, w_h, th_h,
    rho_o, u_o, v_o, w_o, th_o, hh, tth, ttl, qs, sem,
):
    copies = []

    def store(src, dst, b):
        at = pl.ds(b * BR, BR)
        copy = pltpu.make_async_copy(src.at[at], dst.at[at], sem.at[len(copies)])
        copy.start()
        copies.append(copy)

    def extra(k, x, here):
        own = pl.ds(x * N, N)
        west = grid[k, pl.ds(row(x - 1, 0), N), :]
        south = grid[k, pl.ds(row(x, -1), N), :]
        u_o[own, lanes(k)] = us[k, own, :] + (here - west)
        v_o[own, lanes(k)] = vs[k, x, pl.ds(0, N), :] + (here - south)

    def finish(b):
        at = pl.ds(b * BR, BR)
        upward = qs[b % 2, :, pl.ds(0, LV)]
        diff = vertical(upward)
        w_o[at, :] = upward
        th_o[at, :] = qs[b % 2, :, pl.ds(LV, LV)]
        for k in HALVES:
            div = hh[k, at, :] + diff[:, k * LANES : (k + 1) * LANES]
            rho_o[at, lanes(k)] = rho[k, at, :] - courant * div
        store(u_o, u_h, b)
        store(v_o, v_h, b)
        store(rho_o, rho_h, b)
        store(w_o, w_h, b)
        store(th_o, th_h, b)

    pipeline(grid, h0, th, hh, tth, ttl, wh, wl, mh, ml, qs, finish, extra)
    for copy in copies:
        copy.wait()


def kernel(
    rho_h, u_h, v_h, w_h, th_h, cf_h, m_h,
    rho, us, vs, th, h0, mh, ml, wh, wl, gb,
    ws, cf, cc, hh, ms, tth, ttl, qs, ga,
    bth, bxh, bxl, bh0, bh, bcc, bg1,
    cs, cr, ss, sr, gs, gr, ks, kr,
    lsem, csem, crem, ssem, srem, gsem, grem, ksem, krem,
):
    gx = lax.axis_index("gx")
    gy = lax.axis_index("gy")
    nx = lax.axis_size("gx")
    ny = lax.axis_size("gy")
    xm, xp = lax.rem(gx + nx - 1, nx), lax.rem(gx + 1, nx)
    ym, yp = lax.rem(gy + ny - 1, ny), lax.rem(gy + 1, ny)
    side_to = ((xp, gy), (xm, gy), (gx, yp), (gx, ym))
    corner_to = ((xp, yp), (xp, ym), (xm, yp), (xm, ym))

    loads = []

    def load(src, dst):
        copy = pltpu.make_async_copy(src, dst, lsem.at[len(loads)])
        copy.start()
        loads.append(copy)
        return copy

    load_th = [load(th_h.at[:, lanes(k)], th.at[k]) for k in HALVES]
    load_cf = load(cf_h, cf)
    load_u = [load(u_h.at[:, lanes(k)], us.at[k, pl.ds(0, ROWS)]) for k in HALVES]
    load_v = [load(v_h.at[:, :, lanes(k)], vs.at[k, :, pl.ds(0, N)]) for k in HALVES]

    barrier = pltpu.get_barrier_semaphore()
    for to in side_to + corner_to:
        pl.semaphore_signal(barrier, inc=1, device_id=to, device_id_type=MESH)

    def grid_of(n):
        return ga if n % 2 == 1 else gb

    vflat = vs.reshape(2, N * STRIDE, LANES)
    for k in HALVES:
        us[k, pl.ds(ROWS, N), :] = jnp.zeros((N, LANES), f32)
        vs[k, :, pl.ds(N, STRIDE - N), :] = jnp.zeros((N, STRIDE - N, LANES), f32)
    ks[...] = jnp.zeros_like(ks)

    for copy in load_th:
        copy.wait()
    load_cf.wait()
    load_w = [load(w_h.at[:, lanes(k)], ws.at[k]) for k in HALVES]
    load_m = load(m_h, ms)
    load_rho = [load(rho_h.at[:, lanes(k)], rho.at[k]) for k in HALVES]

    def first_g(b, carry):
        at = pl.ds(pl.multiple_of(b * BR, BR), BR)
        for k in HALVES:
            c = -courant * cf[at, lanes(k)].astype(f32)
            cc[k, at, :] = c
            g = c * th[k, at, :]
            for i in range(BX):
                ga[k, pl.ds(pl.multiple_of((b * BX + i + 2) * STRIDE + 8, 8), N), :] = g[i * N : (i + 1) * N]
        return carry

    lax.fori_loop(0, BLOCKS, first_g, 0)
    for copy in load_u + load_v:
        copy.wait()
    for k in HALVES:
        for s in range(4):
            cs[s, 0, k] = ga[k, line(FIRST[s]), :]
        cs[1, 1, k] = us[k, pl.ds(0, N), :]
        cs[3, 1, k] = vflat[k, pl.ds(0, N, STRIDE), :]
        for c in range(4):
            x, y = CORNER_FROM[c]
            ks[0, c, pl.ds(k, 1), :] = ga[k, pl.ds(row(x, y), 1), :]
            ks[0, c, pl.ds(2 + k, 1), :] = us[k, pl.ds(x * N + y, 1), :]
            ks[0, c, pl.ds(4 + k, 1), :] = vflat[k, pl.ds(x * STRIDE + y, 1), :]

    pl.semaphore_wait(barrier, 8)

    def send(src, dst, sent, got, to):
        return pltpu.make_async_remote_copy(
            src_ref=src, dst_ref=dst, send_sem=sent, recv_sem=got,
            device_id=to, device_id_type=MESH,
        )

    def critical(s):
        part = pl.ds(0, 1 + s % 2)
        return send(cs.at[s, part], cr.at[s, part], csem.at[s], crem.at[s], side_to[s])

    def second(s):
        return send(ss.at[s], sr.at[s], ssem.at[s], srem.at[s], side_to[s])

    def side(slot, s):
        return send(gs.at[slot, s], gr.at[slot, s], gsem.at[slot, s], grem.at[slot, s], side_to[s])

    def corner(slot, c):
        return send(ks.at[slot, c], kr.at[slot, c], ksem.at[slot, c], krem.at[slot, c], corner_to[c])

    for s in range(4):
        critical(s).start()
    for c in range(4):
        corner(0, c).start()

    def first_h(x, carry):
        at = pl.ds(pl.multiple_of(x * N, N), N)
        nxt = pl.ds(pl.multiple_of(x * N + N, N), N)
        for k in HALVES:
            h0[k, at, :] = (us[k, nxt, :] - us[k, at, :]) + (
                vs[k, x, pl.ds(1, N), :] - vs[k, x, pl.ds(0, N), :]
            )
        return carry

    lax.fori_loop(0, N, first_h, 0)
    for copy in load_w:
        copy.wait()
    for k in HALVES:
        for s in range(4):
            edge = compact(FIRST[s])
            inner = ga[k, line(SECOND[s]), :]
            bg1[k, pl.ds(s * N, N), :] = inner
            ss[s, 0, k] = ws[k, edge, :]
            ss[s, 1, k] = cc[k, edge, :]
            ss[s, 2, k] = h0[k, edge, :] + inner
    for s in range(4):
        second(s).start()

    def first_w(b, carry):
        at = pl.ds(pl.multiple_of(b * BR, BR), BR)
        for k in HALVES:
            high, low = split(ws[k, at, :])
            wh[at, lanes(k)] = high
            wl[at, lanes(k)] = low
        return carry

    lax.fori_loop(0, BLOCKS, first_w, 0)
    load_m.wait()
    for i in range(4):
        for j in range(4):
            high, low = split(ms[pl.ds(i * 128, 128), pl.ds(j * 128, 128)].T)
            mh[pl.ds(j * 128, 128), pl.ds(i * 128, 128)] = high
            ml[pl.ds(j * 128, 128), pl.ds(i * 128, 128)] = low

    own_corners = [pl.ds(x * N + y, 1) for x, y in CORNER_FROM]

    def early_state(s, k):
        at = pl.ds(N * 4 + s * N, N)
        from_main = compact(SECOND[s])
        bth[k, at, :] = th[k, from_main, :]
        bcc[k, at, :] = cc[k, from_main, :]
        high, low = split(ws[k, from_main, :])
        bxh[at, lanes(k)] = high
        bxl[at, lanes(k)] = low

    for k in HALVES:
        for s in range(4):
            early_state(s, k)
        at = pl.ds(8 * N, CORNER_ROWS)
        bth[k, at, :] = corner_rows([th[k, own, :] for own in own_corners])
        bcc[k, at, :] = corner_rows([cc[k, own, :] for own in own_corners])
        high, low = split(corner_rows([ws[k, own, :] for own in own_corners]))
        bxh[at, lanes(k)] = high
        bxl[at, lanes(k)] = low

    for copy in load_rho:
        copy.wait()
    for s in range(4):
        critical(s).wait_recv()
    for k in HALVES:
        for s in range(4):
            ga[k, line(RING[s]), :] = cr[s, 0, k]
        us[k, pl.ds(ROWS, N), :] = cr[1, 1, k]
        last_x = pl.ds(ROWS - N, N)
        h0[k, last_x, :] = h0[k, last_x, :] + cr[1, 1, k]
        last_y = pl.ds(N - 1, N, N)
        h0[k, last_y, :] = h0[k, last_y, :] + cr[3, 1, k]
        for s in range(4):
            bh0[k, pl.ds(N * 4 + s * N, N), :] = h0[k, compact(SECOND[s]), :]
        bh0[k, pl.ds(8 * N, CORNER_ROWS), :] = corner_rows([h0[k, own, :] for own in own_corners])

    def batch(n, edges, base, with_corners):
        grid = grid_of(n)
        at = pl.ds(base, 4 * N + (CORNER_ROWS if with_corners else 0))
        total = []
        for k in HALVES:
            laps, heres = zip(*[laplacian(grid, k, edge) for edge in edges])
            if with_corners:
                more = [corner_laplacian(grid, k, x, y) for x, y in CORNER_FROM]
                laps += (corner_rows([lap for lap, _ in more]),)
                heres += (corner_rows([here for _, here in more]),)
            total.append(jnp.concatenate(heres, axis=0))
            h = bh0[k, at, :] + jnp.concatenate(laps, axis=0)
            bh[k, at, :] = h
            high, low = split(bth[k, at, :] - courant * h)
            bxh[at, pl.ds(LV + k * LANES, LANES)] = high
            bxl[at, pl.ds(LV + k * LANES, LANES)] = low
        q = product(mh, ml, [(bxh[at, :], bxl[at, :], pl.ds(0, 2 * LV))])
        diff = vertical(q[:, :LV])
        out = []
        for k in HALVES:
            part = slice(k * LANES, (k + 1) * LANES)
            high, low = split(q[:, part])
            bxh[at, lanes(k)] = high
            bxl[at, lanes(k)] = low
            theta = q[:, LV + k * LANES : LV + (k + 1) * LANES]
            bth[k, at, :] = theta
            div = bh[k, at, :] + diff[:, part]
            out.append(total[k] + bcc[k, at, :] * theta + damping * div)
        return out

    def early(n, slot):
        out = batch(n, SECOND, 4 * N, True)
        for k in HALVES:
            for s in range(4):
                part = slice(s * N, (s + 1) * N)
                gs[slot, s, k] = out[k][part] - bg1[k, pl.ds(s * N, N), :]
                ks[slot + 1, s, pl.ds(k, 1), :] = out[k][4 * N + s : 4 * N + s + 1]
        for s in range(4):
            side(slot, s).start()
            corner(slot + 1, s).start()

    def ring(n):
        out = batch(n, RING, 0, False)
        grid = grid_of(n + 1)
        for k in HALVES:
            for s in range(4):
                grid[k, line(RING[s]), :] = out[k][s * N : (s + 1) * N]

    def ring_state():
        for s in range(4):
            second(s).wait_recv()
        for c in range(4):
            corner(0, c).wait_recv()
        last = lax.broadcasted_iota(jnp.int32, (N, LANES), 0) == N - 1
        for k in HALVES:
            extra = (
                us[k, pl.ds(0, N), :], None, vflat[k, pl.ds(0, N, STRIDE), :], None,
            )
            end = (kr[0, 1, pl.ds(4 + k, 1), :], kr[0, 3, pl.ds(4 + k, 1), :],
                   kr[0, 2, pl.ds(2 + k, 1), :], kr[0, 3, pl.ds(2 + k, 1), :])
            for s in range(4):
                at = pl.ds(s * N, N)
                coef = sr[s, 1, k]
                bth[k, at, :] = cr[s, 0, k] / coef
                high, low = split(sr[s, 0, k])
                bxh[at, lanes(k)] = high
                bxl[at, lanes(k)] = low
                bcc[k, at, :] = coef
                h = sr[s, 2, k] + jnp.where(last, end[s], 0.0)
                bh0[k, at, :] = h if extra[s] is None else h + extra[s]
                ga[k, line(OUTER[s]), :] = jnp.zeros((N, LANES), f32)
                x, y = CORNER_AT[s]
                ga[k, pl.ds(row(x, y), 1), :] = kr[0, s, pl.ds(k, 1), :]

    def receive(n, slot):
        grid = grid_of(n)
        for s in range(4):
            side(slot, s).wait_recv()
            corner(slot + 1, s).wait_recv()
        for k in HALVES:
            for s in range(4):
                grid[k, line(OUTER[s]), :] = gr[slot, s, k]
                x, y = CORNER_AT[s]
                grid[k, pl.ds(row(x, y), 1), :] = kr[slot + 1, s, pl.ds(k, 1), :]

    def main(n):
        grid, later = grid_of(n), grid_of(n + 1)

        def finish(b):
            at = pl.ds(b * BR, BR)
            upward = qs[b % 2, :, pl.ds(0, LV)]
            diff = vertical(upward)
            for k in HALVES:
                part = slice(k * LANES, (k + 1) * LANES)
                theta = qs[b % 2, :, pl.ds(LV + k * LANES, LANES)]
                div = hh[k, at, :] + diff[:, part]
                rho[k, at, :] = rho[k, at, :] - courant * div
                th[k, at, :] = theta
                high, low = split(upward[:, part])
                wh[at, lanes(k)] = high
                wl[at, lanes(k)] = low
                g = cc[k, at, :] * theta + damping * div
                for i in range(BX):
                    own = pl.ds(row(b * BX + i, 0), N)
                    later[k, own, :] = grid[k, own, :] + g[i * N : (i + 1) * N]

        pipeline(grid, h0, th, hh, tth, ttl, wh, wl, mh, ml, qs, finish)

    early(1, 0)
    main(1)
    ring_state()
    ring(1)

    for n in range(2, SUBSTEPS):
        if n < SUBSTEPS - 1:
            early(n, n - 1)
        main(n)
        receive(n, n - 2)
        ring(n)

    for s in range(4):
        critical(s).wait_send()
        second(s).wait_send()
        corner(0, s).wait_send()
        for slot in range(MESSAGES):
            side(slot, s).wait_send()
            corner(slot + 1, s).wait_send()


def body(density, flux_east, flux_north, flux_up, theta_pert, sound_coef, vert_inverse):
    flat = (ROWS, LV)
    half_shape = (2, ROWS, LANES)
    half = pltpu.VMEM(half_shape, f32)
    operand = pltpu.VMEM(flat, bf16)
    plane = (2, N, LANES)
    batch_half = pltpu.VMEM((2, 8 * N + CORNER_ROWS, LANES), f32)
    batch_operand = pltpu.VMEM((8 * N + CORNER_ROWS, 2 * LV), bf16)
    hbm = pl.BlockSpec(memory_space=pltpu.HBM)
    vmem = pl.BlockSpec(memory_space=pltpu.VMEM)
    dma = pltpu.SemaphoreType.DMA
    shape = jax.ShapeDtypeStruct
    state = pl.pallas_call(
        kernel,
        out_shape=[
            shape(half_shape, f32),
            shape((2, ROWS + N, LANES), f32),
            shape((2, N, STRIDE, LANES), f32),
            shape(half_shape, f32),
            shape(half_shape, f32),
            shape((2 * LV, 2 * LV), bf16),
            shape((2 * LV, 2 * LV), bf16),
            shape(flat, bf16),
            shape(flat, bf16),
            shape((2, PADDED, LANES), f32),
        ],
        in_specs=[hbm] * 7,
        out_specs=[vmem] * 10,
        scratch_shapes=[
            half,
            operand,
            half,
            half,
            pltpu.VMEM((2 * LV, 2 * LV), f32),
            operand,
            operand,
            pltpu.VMEM((2, BR, 2 * LV), f32),
            pltpu.VMEM((2, PADDED, LANES), f32),
            batch_half,
            batch_operand,
            batch_operand,
            batch_half,
            batch_half,
            batch_half,
            pltpu.VMEM((2, 4 * N, LANES), f32),
            pltpu.VMEM((4, 2) + plane, f32),
            pltpu.VMEM((4, 2) + plane, f32),
            pltpu.VMEM((4, 3) + plane, f32),
            pltpu.VMEM((4, 3) + plane, f32),
            pltpu.VMEM((MESSAGES, 4) + plane, f32),
            pltpu.VMEM((MESSAGES, 4) + plane, f32),
            pltpu.VMEM((MESSAGES + 1, 4, 8, LANES), f32),
            pltpu.VMEM((MESSAGES + 1, 4, 8, LANES), f32),
            dma((12,)),
            dma((4,)), dma((4,)),
            dma((4,)), dma((4,)),
            dma((MESSAGES, 4)), dma((MESSAGES, 4)),
            dma((MESSAGES + 1, 4)), dma((MESSAGES + 1, 4)),
        ],
        compiler_params=pltpu.CompilerParams(
            collective_id=0, has_side_effects=True, vmem_limit_bytes=28 * 1024 * 1024
        ),
    )(*[pltpu.with_memory_space_constraint(array, pltpu.HBM) for array in (
        density.reshape(flat),
        flux_east.reshape(flat),
        flux_north,
        flux_up.reshape(flat),
        theta_pert.reshape(flat),
        sound_coef.reshape(flat),
        vert_inverse,
    )])
    out = pltpu.VMEM(flat, f32)
    outs = pl.pallas_call(
        last_kernel,
        out_shape=[shape(flat, f32)] * 5,
        in_specs=[vmem] * 10,
        out_specs=[hbm] * 5,
        scratch_shapes=[
            out, out, out, out, out, half, operand, operand,
            pltpu.VMEM((2, BR, 2 * LV), f32),
            dma((5 * BLOCKS,)),
        ],
        compiler_params=pltpu.CompilerParams(vmem_limit_bytes=28 * 1024 * 1024),
    )(*state)
    return tuple(out.reshape(N, N, LV) for out in outs)


def solution(mesh):
    block = P("gx", "gy", None)
    return jax.shard_map(
        body,
        mesh=mesh,
        in_specs=(block,) * 6 + (P(),),
        out_specs=(block,) * 5,
        check_vma=False,
    )
```

```python
import jax
import jax.numpy as jnp
from jax import lax
from jax.experimental import pallas as pl
from jax.experimental.pallas import tpu as pltpu
from jax.sharding import PartitionSpec as P

SUBSTEPS = 6
courant = 0.45
damping = 0.1
MESH = pl.DeviceIdType.MESH
f32 = jnp.float32
bf16 = jnp.bfloat16

N = 32
LV = 256
LANES = 128
HALVES = (0, 1)
ROWS = N * N
STRIDE = 40
PADDED = (N + 4) * STRIDE + 8
BX = 8
BR = BX * N
BLOCKS = N // BX
CORNER_ROWS = 16
MESSAGES = SUBSTEPS - 2
RING = (("x", -1), ("x", N), ("y", -1), ("y", N))
FIRST = (("x", N - 1), ("x", 0), ("y", N - 1), ("y", 0))
SECOND = (("x", N - 2), ("x", 1), ("y", N - 2), ("y", 1))
OUTER = (("x", -2), ("x", N + 1), ("y", -2), ("y", N + 1))
CORNER_FROM = ((N - 1, N - 1), (N - 1, 0), (0, N - 1), (0, 0))
CORNER_AT = ((-1, -1), (-1, N), (N, -1), (N, N))


def lanes(half):
    return pl.ds(half * LANES, LANES)


def row(x, y):
    return (x + 2) * STRIDE + 8 + y


def line(side, dx=0, dy=0):
    axis, at = side
    if axis == "x":
        return pl.ds(row(at + dx, dy), N)
    return pl.ds(row(dx, at + dy), N, STRIDE)


def compact(side):
    axis, at = side
    if axis == "x":
        return pl.ds(at * N, N)
    return pl.ds(at, N, N)


def split(value):
    high = value.astype(bf16)
    return high, (value - high.astype(f32)).astype(bf16)


def vertical(upward):
    first = lax.broadcasted_iota(jnp.int32, upward.shape, 1) == 0
    return upward - jnp.where(first, 0.0, pltpu.roll(upward, 1, 1))


def laplacian(grid, k, edge):
    here = grid[k, line(edge), :]
    around = (grid[k, line(edge, -1), :] + grid[k, line(edge, 1), :]) + (
        grid[k, line(edge, 0, -1), :] + grid[k, line(edge, 0, 1), :]
    )
    return around - 4.0 * here, here


def corner_laplacian(grid, k, x, y):
    at = [grid[k, pl.ds(row(x + i, y + j), 1), :] for i, j in ((0, 0), (-1, 0), (1, 0), (0, -1), (0, 1))]
    return (at[1] + at[2]) + (at[3] + at[4]) - 4.0 * at[0], at[0]


def corner_rows(rows):
    return jnp.concatenate(rows + [jnp.zeros((CORNER_ROWS - 4, LANES), f32)], axis=0)


def product(mh, ml, parts):
    total = None
    for high, low, depth in parts:
        for left, right in ((high, mh), (low, mh), (high, ml)):
            term = jnp.dot(left, right[depth, :], preferred_element_type=f32)
            total = term if total is None else total + term
    return total


def pipeline(grid, h0, th, hh, tth, ttl, wh, wl, mh, ml, qs, finish, extra=None):
    def prepare(b):
        at = pl.ds(b * BR, BR)
        for k in HALVES:
            laps = []
            for i in range(BX):
                lap, here = laplacian(grid, k, ("x", b * BX + i))
                laps.append(lap)
                if extra is not None:
                    extra(k, b * BX + i, here)
            h = h0[k, at, :] + jnp.concatenate(laps, axis=0)
            hh[k, at, :] = h
            high, low = split(th[k, at, :] - courant * h)
            tth[at, lanes(k)] = high
            ttl[at, lanes(k)] = low

    def multiply(b):
        at = pl.ds(b * BR, BR)
        qs[b % 2] = product(mh, ml, [
            (wh[at, :], wl[at, :], pl.ds(0, LV)),
            (tth[at, :], ttl[at, :], pl.ds(LV, LV)),
        ])

    prepare(0)
    for b in range(BLOCKS):
        if b + 1 < BLOCKS:
            prepare(b + 1)
        multiply(b)
        if b > 0:
            finish(b - 1)
    finish(BLOCKS - 1)


def last_kernel(
    rho, us, vs, th, h0, mh, ml, wh, wl, grid,
    rho_h, u_h, v_h, w_h, th_h,
    rho_o, u_o, v_o, w_o, th_o, hh, tth, ttl, qs, sem,
):
    copies = []

    def store(src, dst, b):
        at = pl.ds(b * BR, BR)
        copy = pltpu.make_async_copy(src.at[at], dst.at[at], sem.at[len(copies)])
        copy.start()
        copies.append(copy)

    def extra(k, x, here):
        own = pl.ds(x * N, N)
        west = grid[k, pl.ds(row(x - 1, 0), N), :]
        south = grid[k, pl.ds(row(x, -1), N), :]
        u_o[own, lanes(k)] = us[k, own, :] + (here - west)
        v_o[own, lanes(k)] = vs[k, x, pl.ds(0, N), :] + (here - south)

    def finish(b):
        at = pl.ds(b * BR, BR)
        upward = qs[b % 2, :, pl.ds(0, LV)]
        diff = vertical(upward)
        w_o[at, :] = upward
        th_o[at, :] = qs[b % 2, :, pl.ds(LV, LV)]
        for k in HALVES:
            div = hh[k, at, :] + diff[:, k * LANES : (k + 1) * LANES]
            rho_o[at, lanes(k)] = rho[k, at, :] - courant * div
        store(u_o, u_h, b)
        store(v_o, v_h, b)
        store(rho_o, rho_h, b)
        store(w_o, w_h, b)
        store(th_o, th_h, b)

    pipeline(grid, h0, th, hh, tth, ttl, wh, wl, mh, ml, qs, finish, extra)
    for copy in copies:
        copy.wait()


def kernel(
    rho_h, u_h, v_h, w_h, th_h, cf_h, m_h,
    rho, us, vs, th, h0, mh, ml, wh, wl, gb,
    ws, cf, cc, hh, ms, tth, ttl, qs, ga,
    bth, bxh, bxl, bh0, bh, bcc, bg1,
    cs, cr, ss, sr, gs, gr, ks, kr,
    lsem, csem, crem, ssem, srem, gsem, grem, ksem, krem,
):
    gx = lax.axis_index("gx")
    gy = lax.axis_index("gy")
    nx = lax.axis_size("gx")
    ny = lax.axis_size("gy")
    xm, xp = lax.rem(gx + nx - 1, nx), lax.rem(gx + 1, nx)
    ym, yp = lax.rem(gy + ny - 1, ny), lax.rem(gy + 1, ny)
    side_to = ((xp, gy), (xm, gy), (gx, yp), (gx, ym))
    corner_to = ((xp, yp), (xp, ym), (xm, yp), (xm, ym))

    loads = []

    def load(src, dst):
        copy = pltpu.make_async_copy(src, dst, lsem.at[len(loads)])
        copy.start()
        loads.append(copy)
        return copy

    load_th = [load(th_h.at[:, lanes(k)], th.at[k]) for k in HALVES]
    load_cf = load(cf_h, cf)
    load_u = [load(u_h.at[:, lanes(k)], us.at[k, pl.ds(0, ROWS)]) for k in HALVES]
    load_v = [load(v_h.at[:, :, lanes(k)], vs.at[k, :, pl.ds(0, N)]) for k in HALVES]
    load_w = [load(w_h.at[:, lanes(k)], ws.at[k]) for k in HALVES]

    barrier = pltpu.get_barrier_semaphore()
    for to in side_to + corner_to:
        pl.semaphore_signal(barrier, inc=1, device_id=to, device_id_type=MESH)

    def grid_of(n):
        return ga if n % 2 == 1 else gb

    vflat = vs.reshape(2, N * STRIDE, LANES)
    for k in HALVES:
        us[k, pl.ds(ROWS, N), :] = jnp.zeros((N, LANES), f32)
        vs[k, :, pl.ds(N, STRIDE - N), :] = jnp.zeros((N, STRIDE - N, LANES), f32)
    ks[...] = jnp.zeros_like(ks)

    for copy in load_th:
        copy.wait()
    load_cf.wait()
    load_m = load(m_h, ms)
    load_rho = [load(rho_h.at[:, lanes(k)], rho.at[k]) for k in HALVES]

    def first_g(b, carry):
        at = pl.ds(pl.multiple_of(b * BR, BR), BR)
        for k in HALVES:
            c = -courant * cf[at, lanes(k)].astype(f32)
            cc[k, at, :] = c
            g = c * th[k, at, :]
            for i in range(BX):
                ga[k, pl.ds(pl.multiple_of((b * BX + i + 2) * STRIDE + 8, 8), N), :] = g[i * N : (i + 1) * N]
        return carry

    lax.fori_loop(0, BLOCKS, first_g, 0)
    for copy in load_u + load_v:
        copy.wait()
    for k in HALVES:
        for s in range(4):
            cs[s, 0, k] = ga[k, line(FIRST[s]), :]
        cs[1, 1, k] = us[k, pl.ds(0, N), :]
        cs[3, 1, k] = vflat[k, pl.ds(0, N, STRIDE), :]
        for c in range(4):
            x, y = CORNER_FROM[c]
            ks[0, c, pl.ds(k, 1), :] = ga[k, pl.ds(row(x, y), 1), :]
            ks[0, c, pl.ds(2 + k, 1), :] = us[k, pl.ds(x * N + y, 1), :]
            ks[0, c, pl.ds(4 + k, 1), :] = vflat[k, pl.ds(x * STRIDE + y, 1), :]

    pl.semaphore_wait(barrier, 8)

    def send(src, dst, sent, got, to):
        return pltpu.make_async_remote_copy(
            src_ref=src, dst_ref=dst, send_sem=sent, recv_sem=got,
            device_id=to, device_id_type=MESH,
        )

    def critical(s):
        part = pl.ds(0, 1 + s % 2)
        return send(cs.at[s, part], cr.at[s, part], csem.at[s], crem.at[s], side_to[s])

    def second(s):
        return send(ss.at[s], sr.at[s], ssem.at[s], srem.at[s], side_to[s])

    def side(slot, s):
        return send(gs.at[slot, s], gr.at[slot, s], gsem.at[slot, s], grem.at[slot, s], side_to[s])

    def corner(slot, c):
        return send(ks.at[slot, c], kr.at[slot, c], ksem.at[slot, c], krem.at[slot, c], corner_to[c])

    for s in range(4):
        critical(s).start()
    for c in range(4):
        corner(0, c).start()

    for copy in load_w:
        copy.wait()
    for k in HALVES:
        for s in range(4):
            axis, at = FIRST[s]
            edge = compact(FIRST[s])
            if axis == "x":
                beyond = pl.ds((at + 1) * N, N)
                here, after = vs[k, at, pl.ds(0, N), :], vs[k, at, pl.ds(1, N), :]
            else:
                beyond = pl.ds(N + at, N, N)
                here, after = vflat[k, pl.ds(at, N, STRIDE), :], vflat[k, pl.ds(at + 1, N, STRIDE), :]
            inner = ga[k, line(SECOND[s]), :]
            bg1[k, pl.ds(s * N, N), :] = inner
            ss[s, 0, k] = ws[k, edge, :]
            ss[s, 1, k] = cc[k, edge, :]
            ss[s, 2, k] = (us[k, beyond, :] - us[k, edge, :]) + (after - here) + inner
    for s in range(4):
        second(s).start()

    def first_h(x, carry):
        at = pl.ds(pl.multiple_of(x * N, N), N)
        nxt = pl.ds(pl.multiple_of(x * N + N, N), N)
        for k in HALVES:
            h0[k, at, :] = (us[k, nxt, :] - us[k, at, :]) + (
                vs[k, x, pl.ds(1, N), :] - vs[k, x, pl.ds(0, N), :]
            )
        return carry

    lax.fori_loop(0, N, first_h, 0)

    def first_w(b, carry):
        at = pl.ds(pl.multiple_of(b * BR, BR), BR)
        for k in HALVES:
            high, low = split(ws[k, at, :])
            wh[at, lanes(k)] = high
            wl[at, lanes(k)] = low
        return carry

    lax.fori_loop(0, BLOCKS, first_w, 0)
    load_m.wait()
    for i in range(4):
        for j in range(4):
            high, low = split(ms[pl.ds(i * 128, 128), pl.ds(j * 128, 128)].T)
            mh[pl.ds(j * 128, 128), pl.ds(i * 128, 128)] = high
            ml[pl.ds(j * 128, 128), pl.ds(i * 128, 128)] = low

    own_corners = [pl.ds(x * N + y, 1) for x, y in CORNER_FROM]

    def early_state(s, k):
        at = pl.ds(N * 4 + s * N, N)
        from_main = compact(SECOND[s])
        bth[k, at, :] = th[k, from_main, :]
        bcc[k, at, :] = cc[k, from_main, :]
        high, low = split(ws[k, from_main, :])
        bxh[at, lanes(k)] = high
        bxl[at, lanes(k)] = low

    for k in HALVES:
        for s in range(4):
            early_state(s, k)
        at = pl.ds(8 * N, CORNER_ROWS)
        bth[k, at, :] = corner_rows([th[k, own, :] for own in own_corners])
        bcc[k, at, :] = corner_rows([cc[k, own, :] for own in own_corners])
        high, low = split(corner_rows([ws[k, own, :] for own in own_corners]))
        bxh[at, lanes(k)] = high
        bxl[at, lanes(k)] = low

    for copy in load_rho:
        copy.wait()
    for s in range(4):
        critical(s).wait_recv()
    for k in HALVES:
        for s in range(4):
            ga[k, line(RING[s]), :] = cr[s, 0, k]
        us[k, pl.ds(ROWS, N), :] = cr[1, 1, k]
        last_x = pl.ds(ROWS - N, N)
        h0[k, last_x, :] = h0[k, last_x, :] + cr[1, 1, k]
        last_y = pl.ds(N - 1, N, N)
        h0[k, last_y, :] = h0[k, last_y, :] + cr[3, 1, k]
        for s in range(4):
            bh0[k, pl.ds(N * 4 + s * N, N), :] = h0[k, compact(SECOND[s]), :]
        bh0[k, pl.ds(8 * N, CORNER_ROWS), :] = corner_rows([h0[k, own, :] for own in own_corners])

    def batch(n, edges, base, with_corners):
        grid = grid_of(n)
        at = pl.ds(base, 4 * N + (CORNER_ROWS if with_corners else 0))
        total = []
        for k in HALVES:
            laps, heres = zip(*[laplacian(grid, k, edge) for edge in edges])
            if with_corners:
                more = [corner_laplacian(grid, k, x, y) for x, y in CORNER_FROM]
                laps += (corner_rows([lap for lap, _ in more]),)
                heres += (corner_rows([here for _, here in more]),)
            total.append(jnp.concatenate(heres, axis=0))
            h = bh0[k, at, :] + jnp.concatenate(laps, axis=0)
            bh[k, at, :] = h
            high, low = split(bth[k, at, :] - courant * h)
            bxh[at, pl.ds(LV + k * LANES, LANES)] = high
            bxl[at, pl.ds(LV + k * LANES, LANES)] = low
        q = product(mh, ml, [(bxh[at, :], bxl[at, :], pl.ds(0, 2 * LV))])
        diff = vertical(q[:, :LV])
        out = []
        for k in HALVES:
            part = slice(k * LANES, (k + 1) * LANES)
            high, low = split(q[:, part])
            bxh[at, lanes(k)] = high
            bxl[at, lanes(k)] = low
            theta = q[:, LV + k * LANES : LV + (k + 1) * LANES]
            bth[k, at, :] = theta
            div = bh[k, at, :] + diff[:, part]
            out.append(total[k] + bcc[k, at, :] * theta + damping * div)
        return out

    def early(n, slot):
        out = batch(n, SECOND, 4 * N, True)
        for k in HALVES:
            for s in range(4):
                part = slice(s * N, (s + 1) * N)
                gs[slot, s, k] = out[k][part] - bg1[k, pl.ds(s * N, N), :]
                ks[slot + 1, s, pl.ds(k, 1), :] = out[k][4 * N + s : 4 * N + s + 1]
        for c in range(4):
            corner(slot + 1, c).start()
        for s in range(4):
            side(slot, s).start()

    def ring(n):
        out = batch(n, RING, 0, False)
        grid = grid_of(n + 1)
        for k in HALVES:
            for s in range(4):
                grid[k, line(RING[s]), :] = out[k][s * N : (s + 1) * N]

    def ring_state():
        for s in range(4):
            second(s).wait_recv()
        for c in range(4):
            corner(0, c).wait_recv()
        last = lax.broadcasted_iota(jnp.int32, (N, LANES), 0) == N - 1
        for k in HALVES:
            extra = (
                us[k, pl.ds(0, N), :], None, vflat[k, pl.ds(0, N, STRIDE), :], None,
            )
            end = (kr[0, 1, pl.ds(4 + k, 1), :], kr[0, 3, pl.ds(4 + k, 1), :],
                   kr[0, 2, pl.ds(2 + k, 1), :], kr[0, 3, pl.ds(2 + k, 1), :])
            for s in range(4):
                at = pl.ds(s * N, N)
                coef = sr[s, 1, k]
                bth[k, at, :] = cr[s, 0, k] / coef
                high, low = split(sr[s, 0, k])
                bxh[at, lanes(k)] = high
                bxl[at, lanes(k)] = low
                bcc[k, at, :] = coef
                h = sr[s, 2, k] + jnp.where(last, end[s], 0.0)
                bh0[k, at, :] = h if extra[s] is None else h + extra[s]
                ga[k, line(OUTER[s]), :] = jnp.zeros((N, LANES), f32)
                x, y = CORNER_AT[s]
                ga[k, pl.ds(row(x, y), 1), :] = kr[0, s, pl.ds(k, 1), :]

    def receive(n, slot):
        grid = grid_of(n)
        for s in range(4):
            side(slot, s).wait_recv()
            corner(slot + 1, s).wait_recv()
        for k in HALVES:
            for s in range(4):
                grid[k, line(OUTER[s]), :] = gr[slot, s, k]
                x, y = CORNER_AT[s]
                grid[k, pl.ds(row(x, y), 1), :] = kr[slot + 1, s, pl.ds(k, 1), :]

    def main(n):
        grid, later = grid_of(n), grid_of(n + 1)

        def finish(b):
            at = pl.ds(b * BR, BR)
            upward = qs[b % 2, :, pl.ds(0, LV)]
            diff = vertical(upward)
            for k in HALVES:
                part = slice(k * LANES, (k + 1) * LANES)
                theta = qs[b % 2, :, pl.ds(LV + k * LANES, LANES)]
                div = hh[k, at, :] + diff[:, part]
                rho[k, at, :] = rho[k, at, :] - courant * div
                th[k, at, :] = theta
                high, low = split(upward[:, part])
                wh[at, lanes(k)] = high
                wl[at, lanes(k)] = low
                g = cc[k, at, :] * theta + damping * div
                for i in range(BX):
                    own = pl.ds(row(b * BX + i, 0), N)
                    later[k, own, :] = grid[k, own, :] + g[i * N : (i + 1) * N]

        pipeline(grid, h0, th, hh, tth, ttl, wh, wl, mh, ml, qs, finish)

    early(1, 0)
    main(1)
    ring_state()
    ring(1)

    for n in range(2, SUBSTEPS):
        if n < SUBSTEPS - 1:
            early(n, n - 1)
        main(n)
        receive(n, n - 2)
        ring(n)

    for s in range(4):
        critical(s).wait_send()
        second(s).wait_send()
        corner(0, s).wait_send()
        for slot in range(MESSAGES):
            side(slot, s).wait_send()
            corner(slot + 1, s).wait_send()


def body(density, flux_east, flux_north, flux_up, theta_pert, sound_coef, vert_inverse):
    flat = (ROWS, LV)
    half_shape = (2, ROWS, LANES)
    half = pltpu.VMEM(half_shape, f32)
    operand = pltpu.VMEM(flat, bf16)
    plane = (2, N, LANES)
    batch_half = pltpu.VMEM((2, 8 * N + CORNER_ROWS, LANES), f32)
    batch_operand = pltpu.VMEM((8 * N + CORNER_ROWS, 2 * LV), bf16)
    hbm = pl.BlockSpec(memory_space=pltpu.HBM)
    vmem = pl.BlockSpec(memory_space=pltpu.VMEM)
    dma = pltpu.SemaphoreType.DMA
    shape = jax.ShapeDtypeStruct
    state = pl.pallas_call(
        kernel,
        out_shape=[
            shape(half_shape, f32),
            shape((2, ROWS + N, LANES), f32),
            shape((2, N, STRIDE, LANES), f32),
            shape(half_shape, f32),
            shape(half_shape, f32),
            shape((2 * LV, 2 * LV), bf16),
            shape((2 * LV, 2 * LV), bf16),
            shape(flat, bf16),
            shape(flat, bf16),
            shape((2, PADDED, LANES), f32),
        ],
        in_specs=[hbm] * 7,
        out_specs=[vmem] * 10,
        scratch_shapes=[
            half,
            operand,
            half,
            half,
            pltpu.VMEM((2 * LV, 2 * LV), f32),
            operand,
            operand,
            pltpu.VMEM((2, BR, 2 * LV), f32),
            pltpu.VMEM((2, PADDED, LANES), f32),
            batch_half,
            batch_operand,
            batch_operand,
            batch_half,
            batch_half,
            batch_half,
            pltpu.VMEM((2, 4 * N, LANES), f32),
            pltpu.VMEM((4, 2) + plane, f32),
            pltpu.VMEM((4, 2) + plane, f32),
            pltpu.VMEM((4, 3) + plane, f32),
            pltpu.VMEM((4, 3) + plane, f32),
            pltpu.VMEM((MESSAGES, 4) + plane, f32),
            pltpu.VMEM((MESSAGES, 4) + plane, f32),
            pltpu.VMEM((MESSAGES + 1, 4, 8, LANES), f32),
            pltpu.VMEM((MESSAGES + 1, 4, 8, LANES), f32),
            dma((12,)),
            dma((4,)), dma((4,)),
            dma((4,)), dma((4,)),
            dma((MESSAGES, 4)), dma((MESSAGES, 4)),
            dma((MESSAGES + 1, 4)), dma((MESSAGES + 1, 4)),
        ],
        compiler_params=pltpu.CompilerParams(
            collective_id=0, has_side_effects=True, vmem_limit_bytes=28 * 1024 * 1024
        ),
    )(*[pltpu.with_memory_space_constraint(array, pltpu.HBM) for array in (
        density.reshape(flat),
        flux_east.reshape(flat),
        flux_north,
        flux_up.reshape(flat),
        theta_pert.reshape(flat),
        sound_coef.reshape(flat),
        vert_inverse,
    )])
    out = pltpu.VMEM(flat, f32)
    outs = pl.pallas_call(
        last_kernel,
        out_shape=[shape(flat, f32)] * 5,
        in_specs=[vmem] * 10,
        out_specs=[hbm] * 5,
        scratch_shapes=[
            out, out, out, out, out, half, operand, operand,
            pltpu.VMEM((2, BR, 2 * LV), f32),
            dma((5 * BLOCKS,)),
        ],
        compiler_params=pltpu.CompilerParams(vmem_limit_bytes=28 * 1024 * 1024),
    )(*state)
    return tuple(out.reshape(N, N, LV) for out in outs)


def solution(mesh):
    block = P("gx", "gy", None)
    return jax.shard_map(
        body,
        mesh=mesh,
        in_specs=(block,) * 6 + (P(),),
        out_specs=(block,) * 5,
        check_vma=False,
    )
```

```python
import jax
import jax.numpy as jnp
from jax import lax
from jax.experimental import pallas as pl
from jax.experimental.pallas import tpu as pltpu
from jax.sharding import PartitionSpec as P

SUBSTEPS = 6
courant = 0.45
damping = 0.1
MESH = pl.DeviceIdType.MESH
f32 = jnp.float32
bf16 = jnp.bfloat16

N = 32
LV = 256
LANES = 128
HALVES = (0, 1)
ROWS = N * N
STRIDE = 40
PADDED = (N + 4) * STRIDE + 8
BX = 8
BR = BX * N
BLOCKS = N // BX
CORNER_ROWS = 16
MESSAGES = SUBSTEPS - 2
RING = (("x", -1), ("x", N), ("y", -1), ("y", N))
FIRST = (("x", N - 1), ("x", 0), ("y", N - 1), ("y", 0))
SECOND = (("x", N - 2), ("x", 1), ("y", N - 2), ("y", 1))
OUTER = (("x", -2), ("x", N + 1), ("y", -2), ("y", N + 1))
CORNER_FROM = ((N - 1, N - 1), (N - 1, 0), (0, N - 1), (0, 0))
CORNER_AT = ((-1, -1), (-1, N), (N, -1), (N, N))


def lanes(half):
    return pl.ds(half * LANES, LANES)


def row(x, y):
    return (x + 2) * STRIDE + 8 + y


def line(side, dx=0, dy=0):
    axis, at = side
    if axis == "x":
        return pl.ds(row(at + dx, dy), N)
    return pl.ds(row(dx, at + dy), N, STRIDE)


def compact(side):
    axis, at = side
    if axis == "x":
        return pl.ds(at * N, N)
    return pl.ds(at, N, N)


def split(value):
    high = value.astype(bf16)
    return high, (value - high.astype(f32)).astype(bf16)


def vertical(upward):
    first = lax.broadcasted_iota(jnp.int32, upward.shape, 1) == 0
    return upward - jnp.where(first, 0.0, pltpu.roll(upward, 1, 1))


def laplacian(grid, k, edge):
    here = grid[k, line(edge), :]
    around = (grid[k, line(edge, -1), :] + grid[k, line(edge, 1), :]) + (
        grid[k, line(edge, 0, -1), :] + grid[k, line(edge, 0, 1), :]
    )
    return around - 4.0 * here, here


def corner_laplacian(grid, k, x, y):
    at = [grid[k, pl.ds(row(x + i, y + j), 1), :] for i, j in ((0, 0), (-1, 0), (1, 0), (0, -1), (0, 1))]
    return (at[1] + at[2]) + (at[3] + at[4]) - 4.0 * at[0], at[0]


def corner_rows(rows):
    return jnp.concatenate(rows + [jnp.zeros((CORNER_ROWS - 4, LANES), f32)], axis=0)


def product(mh, ml, parts):
    total = None
    for high, low, depth in parts:
        for left, right in ((high, mh), (low, mh), (high, ml)):
            term = jnp.dot(left, right[depth, :], preferred_element_type=f32)
            total = term if total is None else total + term
    return total


def pipeline(grid, h0, th, hh, tth, ttl, wh, wl, mh, ml, qs, finish, extra=None, ready=None):
    def prepare(b):
        at = pl.ds(b * BR, BR)
        for k in HALVES:
            laps = []
            for i in range(BX):
                lap, here = laplacian(grid, k, ("x", b * BX + i))
                laps.append(lap)
                if extra is not None:
                    extra(k, b * BX + i, here)
            h = h0[k, at, :] + jnp.concatenate(laps, axis=0)
            hh[k, at, :] = h
            high, low = split(th[k, at, :] - courant * h)
            tth[at, lanes(k)] = high
            ttl[at, lanes(k)] = low

    def multiply(b):
        at = pl.ds(b * BR, BR)
        qs[b % 2] = product(mh, ml, [
            (wh[at, :], wl[at, :], pl.ds(0, LV)),
            (tth[at, :], ttl[at, :], pl.ds(LV, LV)),
        ])

    prepare(0)
    for b in range(BLOCKS):
        if b + 1 < BLOCKS:
            prepare(b + 1)
        multiply(b)
        if ready is not None:
            ready(b)
        if b > 0:
            finish(b - 1)
    finish(BLOCKS - 1)


def last_kernel(
    rho, us, vs, th, h0, mh, ml, wh, wl, grid,
    rho_h, u_h, v_h, w_h, th_h,
    rho_o, u_o, v_o, w_o, th_o, hh, tth, ttl, qs, sem,
):
    copies = []

    def store(src, dst, b):
        at = pl.ds(b * BR, BR)
        copy = pltpu.make_async_copy(src.at[at], dst.at[at], sem.at[len(copies)])
        copy.start()
        copies.append(copy)

    def extra(k, x, here):
        own = pl.ds(x * N, N)
        west = grid[k, pl.ds(row(x - 1, 0), N), :]
        south = grid[k, pl.ds(row(x, -1), N), :]
        u_o[own, lanes(k)] = us[k, own, :] + (here - west)
        v_o[own, lanes(k)] = vs[k, x, pl.ds(0, N), :] + (here - south)

    def finish(b):
        at = pl.ds(b * BR, BR)
        upward = qs[b % 2, :, pl.ds(0, LV)]
        diff = vertical(upward)
        w_o[at, :] = upward
        th_o[at, :] = qs[b % 2, :, pl.ds(LV, LV)]
        for k in HALVES:
            div = hh[k, at, :] + diff[:, k * LANES : (k + 1) * LANES]
            rho_o[at, lanes(k)] = rho[k, at, :] - courant * div
        store(rho_o, rho_h, b)
        store(w_o, w_h, b)
        store(th_o, th_h, b)

    def ready(b):
        store(u_o, u_h, b)
        store(v_o, v_h, b)

    pipeline(grid, h0, th, hh, tth, ttl, wh, wl, mh, ml, qs, finish, extra, ready)
    for copy in copies:
        copy.wait()


def kernel(
    rho_h, u_h, v_h, w_h, th_h, cf_h, m_h,
    rho, us, vs, th, h0, mh, ml, wh, wl, gb,
    ws, cf, cc, hh, ms, tth, ttl, qs, ga,
    bth, bxh, bxl, bh0, bh, bcc, bg1,
    cs, cr, ss, sr, gs, gr, ks, kr,
    lsem, csem, crem, ssem, srem, gsem, grem, ksem, krem,
):
    gx = lax.axis_index("gx")
    gy = lax.axis_index("gy")
    nx = lax.axis_size("gx")
    ny = lax.axis_size("gy")
    xm, xp = lax.rem(gx + nx - 1, nx), lax.rem(gx + 1, nx)
    ym, yp = lax.rem(gy + ny - 1, ny), lax.rem(gy + 1, ny)
    side_to = ((xp, gy), (xm, gy), (gx, yp), (gx, ym))
    corner_to = ((xp, yp), (xp, ym), (xm, yp), (xm, ym))

    loads = []

    def load(src, dst):
        copy = pltpu.make_async_copy(src, dst, lsem.at[len(loads)])
        copy.start()
        loads.append(copy)
        return copy

    load_th = [load(th_h.at[:, lanes(k)], th.at[k]) for k in HALVES]
    load_cf = load(cf_h, cf)
    load_u = [load(u_h.at[:, lanes(k)], us.at[k, pl.ds(0, ROWS)]) for k in HALVES]
    load_v = [load(v_h.at[:, :, lanes(k)], vs.at[k, :, pl.ds(0, N)]) for k in HALVES]
    load_w = [load(w_h.at[:, lanes(k)], ws.at[k]) for k in HALVES]

    barrier = pltpu.get_barrier_semaphore()
    for to in side_to + corner_to:
        pl.semaphore_signal(barrier, inc=1, device_id=to, device_id_type=MESH)

    def grid_of(n):
        return ga if n % 2 == 1 else gb

    vflat = vs.reshape(2, N * STRIDE, LANES)
    for k in HALVES:
        us[k, pl.ds(ROWS, N), :] = jnp.zeros((N, LANES), f32)
        vs[k, :, pl.ds(N, STRIDE - N), :] = jnp.zeros((N, STRIDE - N, LANES), f32)
    ks[...] = jnp.zeros_like(ks)

    for copy in load_th:
        copy.wait()
    load_cf.wait()
    load_m = load(m_h, ms)
    load_rho = [load(rho_h.at[:, lanes(k)], rho.at[k]) for k in HALVES]

    def first_g(b, carry):
        at = pl.ds(pl.multiple_of(b * BR, BR), BR)
        for k in HALVES:
            c = -courant * cf[at, lanes(k)].astype(f32)
            cc[k, at, :] = c
            g = c * th[k, at, :]
            for i in range(BX):
                ga[k, pl.ds(pl.multiple_of((b * BX + i + 2) * STRIDE + 8, 8), N), :] = g[i * N : (i + 1) * N]
        return carry

    lax.fori_loop(0, BLOCKS, first_g, 0)
    for copy in load_u + load_v:
        copy.wait()
    for k in HALVES:
        for s in range(4):
            cs[s, 0, k] = ga[k, line(FIRST[s]), :]
        cs[1, 1, k] = us[k, pl.ds(0, N), :]
        cs[3, 1, k] = vflat[k, pl.ds(0, N, STRIDE), :]
        for c in range(4):
            x, y = CORNER_FROM[c]
            ks[0, c, pl.ds(k, 1), :] = ga[k, pl.ds(row(x, y), 1), :]
            ks[0, c, pl.ds(2 + k, 1), :] = us[k, pl.ds(x * N + y, 1), :]
            ks[0, c, pl.ds(4 + k, 1), :] = vflat[k, pl.ds(x * STRIDE + y, 1), :]

    pl.semaphore_wait(barrier, 8)

    def send(src, dst, sent, got, to):
        return pltpu.make_async_remote_copy(
            src_ref=src, dst_ref=dst, send_sem=sent, recv_sem=got,
            device_id=to, device_id_type=MESH,
        )

    def critical(s):
        part = pl.ds(0, 1 + s % 2)
        return send(cs.at[s, part], cr.at[s, part], csem.at[s], crem.at[s], side_to[s])

    def second(s):
        return send(ss.at[s], sr.at[s], ssem.at[s], srem.at[s], side_to[s])

    def side(slot, s):
        return send(gs.at[slot, s], gr.at[slot, s], gsem.at[slot, s], grem.at[slot, s], side_to[s])

    def corner(slot, c):
        return send(ks.at[slot, c], kr.at[slot, c], ksem.at[slot, c], krem.at[slot, c], corner_to[c])

    for s in range(4):
        critical(s).start()
    for c in range(4):
        corner(0, c).start()

    for copy in load_w:
        copy.wait()
    for k in HALVES:
        for s in range(4):
            axis, at = FIRST[s]
            edge = compact(FIRST[s])
            if axis == "x":
                beyond = pl.ds((at + 1) * N, N)
                here, after = vs[k, at, pl.ds(0, N), :], vs[k, at, pl.ds(1, N), :]
            else:
                beyond = pl.ds(N + at, N, N)
                here, after = vflat[k, pl.ds(at, N, STRIDE), :], vflat[k, pl.ds(at + 1, N, STRIDE), :]
            inner = ga[k, line(SECOND[s]), :]
            bg1[k, pl.ds(s * N, N), :] = inner
            ss[s, 0, k] = ws[k, edge, :]
            ss[s, 1, k] = cc[k, edge, :]
            ss[s, 2, k] = (us[k, beyond, :] - us[k, edge, :]) + (after - here) + inner
    for s in range(4):
        second(s).start()

    def first_h(x, carry):
        at = pl.ds(pl.multiple_of(x * N, N), N)
        nxt = pl.ds(pl.multiple_of(x * N + N, N), N)
        for k in HALVES:
            h0[k, at, :] = (us[k, nxt, :] - us[k, at, :]) + (
                vs[k, x, pl.ds(1, N), :] - vs[k, x, pl.ds(0, N), :]
            )
        return carry

    lax.fori_loop(0, N, first_h, 0)

    def first_w(b, carry):
        at = pl.ds(pl.multiple_of(b * BR, BR), BR)
        for k in HALVES:
            high, low = split(ws[k, at, :])
            wh[at, lanes(k)] = high
            wl[at, lanes(k)] = low
        return carry

    lax.fori_loop(0, BLOCKS, first_w, 0)
    load_m.wait()
    for i in range(4):
        for j in range(4):
            high, low = split(ms[pl.ds(i * 128, 128), pl.ds(j * 128, 128)].T)
            mh[pl.ds(j * 128, 128), pl.ds(i * 128, 128)] = high
            ml[pl.ds(j * 128, 128), pl.ds(i * 128, 128)] = low

    own_corners = [pl.ds(x * N + y, 1) for x, y in CORNER_FROM]

    def early_state(s, k):
        at = pl.ds(N * 4 + s * N, N)
        from_main = compact(SECOND[s])
        bth[k, at, :] = th[k, from_main, :]
        bcc[k, at, :] = cc[k, from_main, :]
        high, low = split(ws[k, from_main, :])
        bxh[at, lanes(k)] = high
        bxl[at, lanes(k)] = low

    for k in HALVES:
        for s in range(4):
            early_state(s, k)
        at = pl.ds(8 * N, CORNER_ROWS)
        bth[k, at, :] = corner_rows([th[k, own, :] for own in own_corners])
        bcc[k, at, :] = corner_rows([cc[k, own, :] for own in own_corners])
        high, low = split(corner_rows([ws[k, own, :] for own in own_corners]))
        bxh[at, lanes(k)] = high
        bxl[at, lanes(k)] = low

    for copy in load_rho:
        copy.wait()
    for s in range(4):
        critical(s).wait_recv()
    for k in HALVES:
        for s in range(4):
            ga[k, line(RING[s]), :] = cr[s, 0, k]
        us[k, pl.ds(ROWS, N), :] = cr[1, 1, k]
        last_x = pl.ds(ROWS - N, N)
        h0[k, last_x, :] = h0[k, last_x, :] + cr[1, 1, k]
        last_y = pl.ds(N - 1, N, N)
        h0[k, last_y, :] = h0[k, last_y, :] + cr[3, 1, k]
        for s in range(4):
            bh0[k, pl.ds(N * 4 + s * N, N), :] = h0[k, compact(SECOND[s]), :]
        bh0[k, pl.ds(8 * N, CORNER_ROWS), :] = corner_rows([h0[k, own, :] for own in own_corners])

    def batch(n, edges, base, with_corners):
        grid = grid_of(n)
        at = pl.ds(base, 4 * N + (CORNER_ROWS if with_corners else 0))
        total = []
        for k in HALVES:
            laps, heres = zip(*[laplacian(grid, k, edge) for edge in edges])
            if with_corners:
                more = [corner_laplacian(grid, k, x, y) for x, y in CORNER_FROM]
                laps += (corner_rows([lap for lap, _ in more]),)
                heres += (corner_rows([here for _, here in more]),)
            total.append(jnp.concatenate(heres, axis=0))
            h = bh0[k, at, :] + jnp.concatenate(laps, axis=0)
            bh[k, at, :] = h
            high, low = split(bth[k, at, :] - courant * h)
            bxh[at, pl.ds(LV + k * LANES, LANES)] = high
            bxl[at, pl.ds(LV + k * LANES, LANES)] = low
        q = product(mh, ml, [(bxh[at, :], bxl[at, :], pl.ds(0, 2 * LV))])
        diff = vertical(q[:, :LV])
        out = []
        for k in HALVES:
            part = slice(k * LANES, (k + 1) * LANES)
            high, low = split(q[:, part])
            bxh[at, lanes(k)] = high
            bxl[at, lanes(k)] = low
            theta = q[:, LV + k * LANES : LV + (k + 1) * LANES]
            bth[k, at, :] = theta
            div = bh[k, at, :] + diff[:, part]
            out.append(total[k] + bcc[k, at, :] * theta + damping * div)
        return out

    def early(n, slot):
        out = batch(n, SECOND, 4 * N, True)
        for k in HALVES:
            for s in range(4):
                part = slice(s * N, (s + 1) * N)
                gs[slot, s, k] = out[k][part] - bg1[k, pl.ds(s * N, N), :]
                ks[slot + 1, s, pl.ds(k, 1), :] = out[k][4 * N + s : 4 * N + s + 1]
        for c in range(4):
            corner(slot + 1, c).start()
        for s in range(4):
            side(slot, s).start()

    def ring(n):
        out = batch(n, RING, 0, False)
        grid = grid_of(n + 1)
        for k in HALVES:
            for s in range(4):
                grid[k, line(RING[s]), :] = out[k][s * N : (s + 1) * N]

    def ring_state():
        for s in range(4):
            second(s).wait_recv()
        for c in range(4):
            corner(0, c).wait_recv()
        last = lax.broadcasted_iota(jnp.int32, (N, LANES), 0) == N - 1
        for k in HALVES:
            extra = (
                us[k, pl.ds(0, N), :], None, vflat[k, pl.ds(0, N, STRIDE), :], None,
            )
            end = (kr[0, 1, pl.ds(4 + k, 1), :], kr[0, 3, pl.ds(4 + k, 1), :],
                   kr[0, 2, pl.ds(2 + k, 1), :], kr[0, 3, pl.ds(2 + k, 1), :])
            for s in range(4):
                at = pl.ds(s * N, N)
                coef = sr[s, 1, k]
                bth[k, at, :] = cr[s, 0, k] / coef
                high, low = split(sr[s, 0, k])
                bxh[at, lanes(k)] = high
                bxl[at, lanes(k)] = low
                bcc[k, at, :] = coef
                h = sr[s, 2, k] + jnp.where(last, end[s], 0.0)
                bh0[k, at, :] = h if extra[s] is None else h + extra[s]
                ga[k, line(OUTER[s]), :] = jnp.zeros((N, LANES), f32)
                x, y = CORNER_AT[s]
                ga[k, pl.ds(row(x, y), 1), :] = kr[0, s, pl.ds(k, 1), :]

    def receive(n, slot):
        grid = grid_of(n)
        for s in range(4):
            side(slot, s).wait_recv()
            corner(slot + 1, s).wait_recv()
        for k in HALVES:
            for s in range(4):
                grid[k, line(OUTER[s]), :] = gr[slot, s, k]
                x, y = CORNER_AT[s]
                grid[k, pl.ds(row(x, y), 1), :] = kr[slot + 1, s, pl.ds(k, 1), :]

    def main(n):
        grid, later = grid_of(n), grid_of(n + 1)

        def finish(b):
            at = pl.ds(b * BR, BR)
            upward = qs[b % 2, :, pl.ds(0, LV)]
            diff = vertical(upward)
            for k in HALVES:
                part = slice(k * LANES, (k + 1) * LANES)
                theta = qs[b % 2, :, pl.ds(LV + k * LANES, LANES)]
                div = hh[k, at, :] + diff[:, part]
                rho[k, at, :] = rho[k, at, :] - courant * div
                th[k, at, :] = theta
                high, low = split(upward[:, part])
                wh[at, lanes(k)] = high
                wl[at, lanes(k)] = low
                g = cc[k, at, :] * theta + damping * div
                for i in range(BX):
                    own = pl.ds(row(b * BX + i, 0), N)
                    later[k, own, :] = grid[k, own, :] + g[i * N : (i + 1) * N]

        pipeline(grid, h0, th, hh, tth, ttl, wh, wl, mh, ml, qs, finish)

    early(1, 0)
    main(1)
    ring_state()
    ring(1)

    for n in range(2, SUBSTEPS):
        if n < SUBSTEPS - 1:
            early(n, n - 1)
        main(n)
        receive(n, n - 2)
        ring(n)

    for s in range(4):
        critical(s).wait_send()
        second(s).wait_send()
        corner(0, s).wait_send()
        for slot in range(MESSAGES):
            side(slot, s).wait_send()
            corner(slot + 1, s).wait_send()


def body(density, flux_east, flux_north, flux_up, theta_pert, sound_coef, vert_inverse):
    flat = (ROWS, LV)
    half_shape = (2, ROWS, LANES)
    half = pltpu.VMEM(half_shape, f32)
    operand = pltpu.VMEM(flat, bf16)
    plane = (2, N, LANES)
    batch_half = pltpu.VMEM((2, 8 * N + CORNER_ROWS, LANES), f32)
    batch_operand = pltpu.VMEM((8 * N + CORNER_ROWS, 2 * LV), bf16)
    hbm = pl.BlockSpec(memory_space=pltpu.HBM)
    vmem = pl.BlockSpec(memory_space=pltpu.VMEM)
    dma = pltpu.SemaphoreType.DMA
    shape = jax.ShapeDtypeStruct
    state = pl.pallas_call(
        kernel,
        out_shape=[
            shape(half_shape, f32),
            shape((2, ROWS + N, LANES), f32),
            shape((2, N, STRIDE, LANES), f32),
            shape(half_shape, f32),
            shape(half_shape, f32),
            shape((2 * LV, 2 * LV), bf16),
            shape((2 * LV, 2 * LV), bf16),
            shape(flat, bf16),
            shape(flat, bf16),
            shape((2, PADDED, LANES), f32),
        ],
        in_specs=[hbm] * 7,
        out_specs=[vmem] * 10,
        scratch_shapes=[
            half,
            operand,
            half,
            half,
            pltpu.VMEM((2 * LV, 2 * LV), f32),
            operand,
            operand,
            pltpu.VMEM((2, BR, 2 * LV), f32),
            pltpu.VMEM((2, PADDED, LANES), f32),
            batch_half,
            batch_operand,
            batch_operand,
            batch_half,
            batch_half,
            batch_half,
            pltpu.VMEM((2, 4 * N, LANES), f32),
            pltpu.VMEM((4, 2) + plane, f32),
            pltpu.VMEM((4, 2) + plane, f32),
            pltpu.VMEM((4, 3) + plane, f32),
            pltpu.VMEM((4, 3) + plane, f32),
            pltpu.VMEM((MESSAGES, 4) + plane, f32),
            pltpu.VMEM((MESSAGES, 4) + plane, f32),
            pltpu.VMEM((MESSAGES + 1, 4, 8, LANES), f32),
            pltpu.VMEM((MESSAGES + 1, 4, 8, LANES), f32),
            dma((12,)),
            dma((4,)), dma((4,)),
            dma((4,)), dma((4,)),
            dma((MESSAGES, 4)), dma((MESSAGES, 4)),
            dma((MESSAGES + 1, 4)), dma((MESSAGES + 1, 4)),
        ],
        compiler_params=pltpu.CompilerParams(
            collective_id=0, has_side_effects=True, vmem_limit_bytes=28 * 1024 * 1024
        ),
    )(*[pltpu.with_memory_space_constraint(array, pltpu.HBM) for array in (
        density.reshape(flat),
        flux_east.reshape(flat),
        flux_north,
        flux_up.reshape(flat),
        theta_pert.reshape(flat),
        sound_coef.reshape(flat),
        vert_inverse,
    )])
    out = pltpu.VMEM(flat, f32)
    outs = pl.pallas_call(
        last_kernel,
        out_shape=[shape(flat, f32)] * 5,
        in_specs=[vmem] * 10,
        out_specs=[hbm] * 5,
        scratch_shapes=[
            out, out, out, out, out, half, operand, operand,
            pltpu.VMEM((2, BR, 2 * LV), f32),
            dma((5 * BLOCKS,)),
        ],
        compiler_params=pltpu.CompilerParams(vmem_limit_bytes=28 * 1024 * 1024),
    )(*state)
    return tuple(out.reshape(N, N, LV) for out in outs)


def solution(mesh):
    block = P("gx", "gy", None)
    return jax.shard_map(
        body,
        mesh=mesh,
        in_specs=(block,) * 6 + (P(),),
        out_specs=(block,) * 5,
        check_vma=False,
    )
```
